512 devices in a mesh: blk: 64 (over y, z), lay: 8 (over x, core).
Axes of the slice: x: 4, y: 8, z: 8, core: 2. Of those that a mesh axis runs over, the one named last changes fastest.
Arguments:
- matrix_source: float32 [128, 1024, 256], P('lay', 'blk'), may hold values from -6 to 6
- accum: float32 [128, 1024, 256], P('lay', 'blk'), may hold values from 0.02 to 0.5
- faces: float32 [6, 128, 1024, 256], P(None, 'lay', 'blk'), may hold values from 0.03 to 30, as said below
- basis: float32 [4, 128, 1024, 256], P(None, 'lay', 'blk'), may hold values from 0.05 to 0.5
- coarse_diag: float32 [32, 256], P('lay', 'blk'), may hold values from 32 to 128
- coarse_ratio: float32 [4, 32, 256], P(None, 'lay', 'blk'), may hold values from 0.1 to 0.24
- frac_source: float32 [262144], P(('blk', 'lay')), may hold values from -6 to 6
- frac_accum: float32 [262144], P(('blk', 'lay')), may hold values from 0.05 to 0.5
- frac_link: float32 [262144], P(('blk', 'lay')), may hold values from 0.5 to 5
- frac_trans: float32 [2, 262144], P(None, ('blk', 'lay')), may hold values from 0.5 to 5
- frac_cell: int32 [262144], P(('blk', 'lay')), may hold values from 0 to 65535
- frac_peer: int32 [2, 262144], P(None, ('blk', 'lay')), may hold values from 0 to 262143, as said below
- frac_count: int32 [512], P(('blk', 'lay')), may hold values from 1 to 512, as said below
Outputs:
- pressure: float32 [128, 1024, 256], P('lay', 'blk')
- fracture: float32 [262144], P(('blk', 'lay'))
The draws below stay inside these ranges and needn't reach their ends.
Inputs may be any that keep to these rules, and one draw needn't show every extreme that they name: `faces`: the x+ face of a cell equals the x- face of the next cell along the first dimension, likewise y and z. `frac_count`: some owner has exactly 512 live slots in every draw. `frac_peer`: each entry is a live slot (slot index below its owner's count) of the same owner or of the owner just before or after it in the order blk index * 8 + lay index.
All inputs are finite; a program needn't handle non-finite values.
Results may differ from the reference program's by a relative error of at most 0.0001.
Values sent between devices are 32-bit elements; how exact they have to be, the bound alone decides.
A program may use at most 64 MiB of HBM per device.

```python
import math
import jax
import jax.numpy as jnp

CX = 16
CY = 16
CZ = 256
FS = 512
BLOCK = 4
NP = 2
ITERS = 2
GX = 128
GY = 1024
NCX = 32
NCY = 256
FRAC = 262144
N_LAY = 8


def fracture_counts(key):
    devices = FRAC // FS
    first_pick = jax.random.randint(jax.random.fold_in(key, 11), (devices,), 0, FS + 1)
    second_pick = jax.random.randint(jax.random.fold_in(key, 12), (devices,), 0, FS + 1)
    counts = 1 + first_pick * second_pick // (FS + 1)
    busiest = jax.random.randint(jax.random.fold_in(key, 13), (), 0, devices)
    return jnp.where(jnp.arange(devices) == busiest, FS, counts).astype(jnp.int32)


def draw_frac_count(key, part):
    return fracture_counts(key)


def draw_frac_peer(key, part):
    devices = FRAC // FS
    counts = fracture_counts(key)
    owner_device = jnp.arange(FRAC, dtype=jnp.int32) // FS
    offset = jax.random.randint(jax.random.fold_in(key, 21), (NP, FRAC), -1, 2)
    target = jnp.clip(owner_device[None] + offset, 0, devices - 1)
    raw_bits = jax.random.randint(jax.random.fold_in(key, 22), (NP, FRAC), 0, 1 << 30)
    slot_pick = raw_bits % counts[target]
    return (target * FS + slot_pick).astype(jnp.int32)


def draw_faces(key, part):

    def log_draw(salt_value, array_shape, low_value, high_value):
        return jnp.exp(jax.random.uniform(jax.random.fold_in(key, salt_value), array_shape, jnp.float32, jnp.log(low_value), jnp.log(high_value)))
    face_x = log_draw(31, (GX + 1, GY, CZ), 0.1, 10.0)
    face_y = log_draw(32, (GX, GY + 1, CZ), 0.1, 10.0)
    face_z = log_draw(33, (GX, GY, CZ + 1), 0.1, 10.0)
    return jnp.stack([face_x[1:], face_x[:-1], face_y[:, 1:], face_y[:, :-1], face_z[:, :, 1:], face_z[:, :, :-1]]).astype(jnp.float32)


def place_ends(entries, key, least, high):
    longest = entries.shape.index(max(entries.shape))
    spots = []
    for shift in (0, 1):
        where = [jax.random.randint(jax.random.fold_in(key, axis), (), 0, length) for axis, length in enumerate(entries.shape)]
        where[longest] = (where[longest] + shift) % entries.shape[longest]
        spots.append(tuple(where))
    return entries.at[spots[0]].set(least).at[spots[1]].set(high)


def levels(key, shape, cuts, least, largest):
    gain = 1.0
    for position, blocks in cuts:
        draws = jax.random.uniform(jax.random.fold_in(jax.random.fold_in(key, 6), position), (blocks,), jnp.float32, least / len(cuts), largest / len(cuts))
        gain = gain * jnp.repeat(jnp.exp(draws), shape[position] // blocks).reshape((-1,) + (1,) * (len(shape) - 1 - position))
    return gain


def centred(key, dims, deviation, bound, cuts=(), held_as=jnp.bfloat16):
    level = levels(key, dims, cuts, -0.22, 0.18) if cuts else 1.0
    values = jax.random.normal(key, dims, jnp.float32) * deviation * level
    return jnp.minimum(jnp.maximum(values, -bound), bound).astype(held_as)


def setup_inputs(seed: int = 0) -> dict:
    streams_of = jax.random.split(jax.random.key(seed), 14)
    return {
        "matrix_source": centred(streams_of[0], (GX, GY, CZ), 1.0, 6.0, ((0, 8), (1, 64)), jnp.float32),
        "accum": jnp.clip(jnp.exp(math.log(0.5) - 3.218876 * jax.random.uniform(streams_of[1], (GX, GY, CZ), jnp.float32) ** levels(streams_of[1], (GX, GY, CZ), ((0, 8), (1, 64)), -0.2, 0.2)), 0.02, 0.5),
        "faces": draw_faces(jax.random.fold_in(streams_of[13], 71), 0),
        "basis": jnp.clip(0.05 + 0.45 * jax.random.uniform(streams_of[3], (4, GX, GY, CZ), jnp.float32) ** levels(streams_of[3], (4, GX, GY, CZ), ((1, 8), (2, 64)), -0.2, 0.2), 0.05, 0.5),
        "coarse_diag": jnp.clip(32.0 + 96.0 * jax.random.uniform(streams_of[4], (NCX, NCY), jnp.float32) ** levels(streams_of[4], (NCX, NCY), ((0, 8), (1, 64)), -0.2, 0.2), 32.0, 128.0),
        "coarse_ratio": jnp.clip(0.1 + 0.13999999 * jax.random.uniform(streams_of[5], (4, NCX, NCY), jnp.float32) ** levels(streams_of[5], (4, NCX, NCY), ((1, 8), (2, 64)), -0.2, 0.2), 0.1, 0.24),
        "frac_source": centred(streams_of[6], (FRAC,), 1.0, 6.0, ((0, 512),), jnp.float32),
        "frac_accum": jnp.clip(jnp.exp(math.log(0.5) - 2.3025851 * jax.random.uniform(streams_of[7], (FRAC,), jnp.float32) ** levels(streams_of[7], (FRAC,), ((0, 512),), -0.2, 0.2)), 0.05, 0.5),
        "frac_link": jnp.clip(jnp.exp(math.log(5.0) - 2.3025851 * jax.random.uniform(streams_of[8], (FRAC,), jnp.float32) ** levels(streams_of[8], (FRAC,), ((0, 512),), -0.2, 0.2)), 0.5, 5.0),
        "frac_trans": jnp.clip(jnp.exp(math.log(5.0) - 2.3025851 * jax.random.uniform(streams_of[9], (NP, FRAC), jnp.float32) ** levels(streams_of[9], (NP, FRAC), ((1, 512),), -0.2, 0.2)), 0.5, 5.0),
        "frac_cell": place_ends(jax.random.randint(streams_of[10], (FRAC,), 0, CX * CY * CZ), jax.random.fold_in(streams_of[10], 1), 0, (CX * CY * CZ) - 1).astype(jnp.int32),
        "frac_peer": draw_frac_peer(jax.random.fold_in(streams_of[13], 71), 0),
        "frac_count": draw_frac_count(jax.random.fold_in(streams_of[13], 71), 0),
    }


OMEGA = 0.8


def place(block_sums, row_start, col_start):
    return jnp.pad(block_sums, ((row_start, 2 - row_start), (col_start, 2 - col_start)))


def spread(node_terms):
    low_mask = (jnp.arange(BLOCK) < BLOCK // 2).astype(jnp.float32)
    high_mask = 1.0 - low_mask
    x_low = low_mask[None, :, None, None]
    x_high = high_mask[None, :, None, None]
    y_low = low_mask[None, None, None, :]
    y_high = high_mask[None, None, None, :]

    def masked_sum(values, weight):
        return jnp.sum(values * weight, axis=(1, 3))

    spread_sum = place(jnp.sum(node_terms[0], axis=(1, 3)), 1, 1)
    spread_sum = spread_sum + place(masked_sum(node_terms[1], x_low), 0, 1) + place(masked_sum(node_terms[1], x_high), 2, 1)
    spread_sum = spread_sum + place(masked_sum(node_terms[2], y_low), 1, 0) + place(masked_sum(node_terms[2], y_high), 1, 2)
    spread_sum = spread_sum + place(masked_sum(node_terms[3], x_low * y_low), 0, 0) + place(masked_sum(node_terms[3], x_low * y_high), 0, 2)
    spread_sum = spread_sum + place(masked_sum(node_terms[3], x_high * y_low), 2, 0) + place(masked_sum(node_terms[3], x_high * y_high), 2, 2)
    return spread_sum


def node_values(extended):
    node_rows = extended.shape[0] - 2
    node_cols = extended.shape[1] - 2
    low_mask = jnp.arange(BLOCK) < BLOCK // 2
    x_low = low_mask[None, :, None, None]
    y_low = low_mask[None, None, None, :]

    def node_grid(row_start, col_start):
        return extended[row_start:row_start + node_rows, col_start:col_start + node_cols][:, None, :, None]

    full_shape = (node_rows, BLOCK, node_cols, BLOCK)
    centre = jnp.broadcast_to(node_grid(1, 1), full_shape)
    side_x = jnp.broadcast_to(jnp.where(x_low, node_grid(0, 1), node_grid(2, 1)), full_shape)
    side_y = jnp.broadcast_to(jnp.where(y_low, node_grid(1, 0), node_grid(1, 2)), full_shape)
    corner = jnp.broadcast_to(jnp.where(x_low, jnp.where(y_low, node_grid(0, 0), node_grid(0, 2)), jnp.where(y_low, node_grid(2, 0), node_grid(2, 2))), full_shape)
    stacked = jnp.stack([centre, side_x, side_y, corner])
    return stacked.reshape(4, node_rows * BLOCK, node_cols * BLOCK)


def prolong(basis, extended):
    fields = node_values(extended)
    return jnp.sum(basis * fields[..., None], axis=0)


def restrict_terms(basis, residual):
    node_sums = jnp.sum(basis * residual[None], axis=3)
    node_rows = node_sums.shape[1] // BLOCK
    node_cols = node_sums.shape[2] // BLOCK
    return spread(node_sums.reshape(4, node_rows, BLOCK, node_cols, BLOCK))


def coarse_second(first_sweep, first_padded, coarse_ratio):
    neighbours = [first_padded[:-2, 1:-1], first_padded[2:, 1:-1], first_padded[1:-1, :-2], first_padded[1:-1, 2:]]
    second = first_sweep
    for direction in range(4):
        second = second + coarse_ratio[direction] * neighbours[direction]
    return second


def flow_rows(padded, faces, accum):
    centre = padded[1:-1, 1:-1, 1:-1]
    beside = [padded[2:, 1:-1, 1:-1], padded[:-2, 1:-1, 1:-1], padded[1:-1, 2:, 1:-1],
              padded[1:-1, :-2, 1:-1], padded[1:-1, 1:-1, 2:], padded[1:-1, 1:-1, :-2]]
    result = accum * centre
    for direction in range(6):
        result = result + faces[direction] * (centre - beside[direction])
    return result


def matrix_rows(padded, pressure, fracture, faces, accum, cell_index, couple):
    result = flow_rows(padded, faces, accum)
    pressure_at = pressure.reshape(-1)[cell_index]
    link_flux = couple * (pressure_at - fracture)
    linked = jax.ops.segment_sum(link_flux, cell_index, num_segments=pressure.size).reshape(pressure.shape)
    return result + linked, pressure_at


def fracture_rows(fracture, pressure_at, peer_values, frac_accum, couple, frac_trans):
    return frac_accum * fracture + couple * (fracture - pressure_at) + jnp.sum(frac_trans * (fracture[None] - peer_values), axis=0)


def reference(matrix_source, accum, faces, basis, coarse_diag, coarse_ratio, frac_source, frac_accum, frac_link, frac_trans, frac_cell, frac_peer, frac_count):
    slot_index = jnp.arange(FRAC, dtype=jnp.int32)
    owner_device = (slot_index // FS).astype(jnp.int32)
    live_mask = (slot_index % FS < frac_count[owner_device]).astype(jnp.float32)
    couple = live_mask * frac_link
    local_x = frac_cell // (CY * CZ)
    local_y = (frac_cell // CZ) % CY
    local_z = frac_cell % CZ
    global_x = (owner_device % N_LAY) * CX + local_x
    global_y = (owner_device // N_LAY) * CY + local_y
    cell_index = ((global_x * GY + global_y) * CZ + local_z).astype(jnp.int32)
    matrix_diag = accum + jnp.sum(faces, axis=0) + jax.ops.segment_sum(couple, cell_index, num_segments=GX * GY * CZ).reshape(accum.shape)
    frac_diag = frac_accum + couple + jnp.sum(frac_trans, axis=0)
    pressure = jnp.zeros(matrix_source.shape, jnp.float32)
    fracture = jnp.zeros(frac_source.shape, jnp.float32)
    for iteration in range(ITERS):
        rows_now, pressure_at = matrix_rows(jnp.pad(pressure, 1), pressure, fracture, faces, accum, cell_index, couple)
        residual = matrix_source - rows_now
        extended = restrict_terms(basis, residual)
        coarse_rhs = extended[1:-1, 1:-1]
        first_sweep = coarse_rhs / coarse_diag
        second = coarse_second(first_sweep, jnp.pad(first_sweep, 1), coarse_ratio)
        pressure = pressure + prolong(basis, jnp.pad(second, 1))
        rows_now, pressure_at = matrix_rows(jnp.pad(pressure, 1), pressure, fracture, faces, accum, cell_index, couple)
        peer_values = fracture[frac_peer]
        frac_now = fracture_rows(fracture, pressure_at, peer_values, frac_accum, couple, frac_trans)
        pressure = pressure + OMEGA * (matrix_source - rows_now) / matrix_diag
        fracture = fracture + OMEGA * live_mask * (frac_source - frac_now) / frac_diag
    return pressure, fracture
```

```python
import jax
import jax.numpy as jnp
from jax import lax
from jax.experimental import pallas as pl
from jax.experimental.pallas import tpu as pltpu
from jax.sharding import PartitionSpec as P

MESH = pl.DeviceIdType.MESH
F32 = jnp.float32
BF16 = jnp.bfloat16
I32 = jnp.int32

CX = 16
CY = 16
CZ = 256
FS = 512
OMEGA = 0.8
KEEP = 1.0 - OMEGA
LANES = 128

AROUND = ((-1, -1), (-1, 0), (-1, 1), (0, -1), (0, 1), (1, -1), (1, 0), (1, 1))


def iota(shape, dim):
    return lax.broadcasted_iota(I32, shape, dim)


def lane_sum(v):
    return jnp.sum(v, axis=1, keepdims=True)


def row_sum(v):
    return jnp.sum(v, axis=0, keepdims=True)


def fold(v):
    return v[:, :LANES] + v[:, LANES:]


def split(v):
    high = v.astype(BF16)
    return high, (v - high.astype(F32)).astype(BF16)


def dot(a, b, contract_b):
    return lax.dot_general(a, b, (((1,), (contract_b,)), ((), ())), preferred_element_type=F32)


def kernel(
    n_blk,
    n_lay,
    src_h,
    acc_h,
    fac_h,
    bas_h,
    cd_h,
    cr_h,
    fs_h,
    fa_h,
    fl_h,
    ft_h,
    fc_h,
    fp_h,
    cnt_h,
    out_p,
    out_f,
    src,
    acc,
    fac,
    bas,
    cd,
    cr,
    fsrc,
    facc,
    flink,
    ftrans,
    fcell,
    fpeer,
    cnt,
    P0,
    P1,
    wgt,
    zhot,
    ctile,
    snd,
    rcv,
    bxh,
    byh,
    bys,
    pxh,
    pyh,
    pys,
    fsnd,
    frcv,
    load_sem,
    tile_ssem,
    tile_rsem,
    basis_ssem,
    basis_rsem,
    edge_ssem,
    edge_rsem,
    frac_ssem,
    frac_rsem,
):
    b = lax.axis_index("blk")
    l = lax.axis_index("lay")

    def is_there(step):
        i, j = l + step[0], b + step[1]
        return (i >= 0) & (i < n_lay) & (j >= 0) & (j < n_blk)

    def device(step):
        return (b + step[1], l + step[0])

    position = b * n_lay + l
    has_next = position < n_blk * n_lay - 1
    has_prev = position > 0
    next_dev = ((position + 1) // n_lay, lax.rem(position + 1, n_lay))
    prev_dev = ((position - 1) // n_lay, lax.rem(position - 1 + n_lay, n_lay))

    loads = []
    for i, (hbm, vmem) in enumerate(
        (
            (bas_h, bas),
            (src_h, src),
            (cd_h, cd),
            (cr_h, cr),
            (fc_h, fcell),
            (fl_h, flink),
            (cnt_h, cnt),
            (fac_h, fac),
            (acc_h, acc),
            (fs_h, fsrc),
            (fa_h, facc),
            (ft_h, ftrans),
            (fp_h, fpeer),
        )
    ):
        copy = pltpu.make_async_copy(hbm, vmem, load_sem.at[i])
        copy.start()
        loads.append(copy)

    rcv[...] = jnp.zeros(rcv.shape, F32)
    frcv[...] = jnp.zeros(frcv.shape, F32)
    sides = ((3, 4), (1, 6))
    for s in range(2):
        step_x = AROUND[sides[1][s]]
        step_y = AROUND[sides[0][s]]

        @pl.when(jnp.logical_not(is_there(step_x)))
        def _():
            bxh[s] = jnp.zeros((4, CY, CZ), F32)
            pxh[s] = jnp.zeros((CY, CZ), F32)

        @pl.when(jnp.logical_not(is_there(step_y)))
        def _():
            byh[s] = jnp.zeros((4, CX, CZ), F32)
            pyh[s] = jnp.zeros((CX, CZ), F32)

    barrier = pltpu.get_barrier_semaphore()
    count = jnp.int32(0)
    for step in AROUND:
        there = is_there(step)
        count = count + there.astype(I32)

        @pl.when(there)
        def _():
            pl.semaphore_signal(barrier, inc=1, device_id=device(step), device_id_type=MESH)

    for there, dev in ((has_next, next_dev), (has_prev, prev_dev)):
        count = count + there.astype(I32)

        @pl.when(there)
        def _():
            pl.semaphore_signal(barrier, inc=1, device_id=dev, device_id_type=MESH)

    loads[2].wait()
    loads[3].wait()
    ctile[...] = jnp.zeros(ctile.shape, F32)
    ctile[0, 0:4, 0:4] = cd[...]
    for g in range(4):
        ctile[g + 1, 0:4, 0:4] = cr[g]
    own_static = jnp.zeros((8, LANES), F32)
    for g in range(5):
        own_static = own_static + pltpu.roll(pltpu.roll(ctile[g], 2, axis=0), 8 * g + 2, axis=1)
    snd[0] = own_static

    for s in range(2):
        outer = (15 + 8) if s else 8
        P0[:, outer + (1 if s else -1), :] = jnp.zeros((CX + 2, CZ), F32)
        P1[:, outer + (1 if s else -1), :] = jnp.zeros((CX + 2, CZ), F32)
        P1[17 if s else 0] = jnp.zeros((32, CZ), F32)

    pl.semaphore_wait(barrier, count)

    def tile_copy(kind, i):
        return pltpu.make_async_remote_copy(
            src_ref=snd.at[kind],
            dst_ref=rcv.at[kind, 7 - i],
            send_sem=tile_ssem.at[kind, i],
            recv_sem=tile_rsem.at[kind, 7 - i],
            device_id=device(AROUND[i]),
            device_id_type=MESH,
        )

    def tile_arrival(kind, i):
        return pltpu.make_async_remote_copy(
            src_ref=snd.at[kind],
            dst_ref=rcv.at[kind, i],
            send_sem=tile_ssem.at[kind, i],
            recv_sem=tile_rsem.at[kind, i],
            device_id=device(AROUND[i]),
            device_id_type=MESH,
        )

    def send_tile(kind):
        for i in range(8):

            @pl.when(is_there(AROUND[i]))
            def _():
                tile_copy(kind, i).start()

    def await_tile(kind):
        for i in range(8):

            @pl.when(is_there(AROUND[i]))
            def _():
                tile_arrival(kind, i).wait_recv()

    def side_copy(source, target, ssem, rsem, axis, s, arrival=False):
        slot = s if arrival else 1 - s
        return pltpu.make_async_remote_copy(
            src_ref=source,
            dst_ref=target.at[slot],
            send_sem=ssem.at[axis, s],
            recv_sem=rsem.at[axis, slot],
            device_id=device(AROUND[sides[axis][s]]),
            device_id_type=MESH,
        )

    def basis_copy(axis, s, arrival=False):
        source = bas.at[:, 15 * s] if axis else bys.at[s]
        return side_copy(source, bxh if axis else byh, basis_ssem, basis_rsem, axis, s, arrival)

    def edge_copy(axis, s, arrival=False):
        source = P1.at[16 if s else 1, 8:24] if axis else pys.at[s]
        return side_copy(source, pxh if axis else pyh, edge_ssem, edge_rsem, axis, s, arrival)

    def on_sides(make, axis, act):
        for s in range(2):

            @pl.when(is_there(AROUND[sides[axis][s]]))
            def _():
                act(make(axis, s))

    send_tile(0)

    q = iota((32, LANES), 0)
    lane32 = iota((32, LANES), 1)
    y = lax.rem(q, 16)
    col = jnp.where(q < 16, y // 4 + 2, jnp.where(lax.rem(y, 4) < 2, y // 4 + 1, y // 4 + 3))
    to_col = (lane32 == col).astype(F32)
    sub8 = iota((8, LANES), 0)
    lane8 = iota((8, LANES), 1)
    low_lane = lax.rem(lane8, 8) < 4
    x16 = iota((16, LANES), 0)
    lane16 = iota((16, LANES), 1)
    row_c = x16 // 4 + 2
    row_s = jnp.where(lax.rem(x16, 4) < 2, x16 // 4 + 1, x16 // 4 + 3)
    x_wide = iota((16, CZ), 0)

    def rows_of_half(h):
        return h // 2 + 1, (h // 2 if h % 2 == 0 else h // 2 + 2)

    def pack_rows(row):
        value = jnp.broadcast_to(row(0), (16, CZ))
        for x in range(1, 16):
            value = jnp.where(x_wide == x, jnp.broadcast_to(row(x), (16, CZ)), value)
        return value

    def restrict(residual_row, x_planes, y_planes):
        centre = [None] * 6
        beside = [None] * 6

        def add(into, r, value):
            into[r] = value if into[r] is None else into[r] + value

        for h in range(8):
            first, second = residual_row(2 * h), residual_row(2 * h + 1)
            rc, rs = rows_of_half(h)
            for k, (into, r) in enumerate(((centre, rc), (centre, rs), (beside, rc), (beside, rs))):
                add(into, r, fold(bas[k, 2 * h] * first + bas[k, 2 * h + 1] * second))
        for s, plane in enumerate(x_planes):
            rc, rs = (5, 4) if s else (0, 1)
            for k, (into, r) in enumerate(((centre, rc), (centre, rs), (beside, rc), (beside, rs))):
                add(into, r, fold(bxh[s, k] * plane))
        tile = jnp.zeros((8, LANES), F32)
        y_c = jnp.zeros((16, LANES), F32)
        y_s = jnp.zeros((16, LANES), F32)
        for s, plane in enumerate(y_planes):
            near, far = (5, 6) if s else (2, 1)
            for k in range(4):
                value = lane_sum(fold(byh[s, k] * plane))
                placed = jnp.where(lane16 == (far if k < 2 else near), value, 0.0)
                if k % 2 == 0:
                    y_c = y_c + placed
                else:
                    y_s = y_s + placed
        for r in range(6):
            value = lane_sum(jnp.concatenate([centre[r], beside[r]], axis=0))
            line = row_sum(value * to_col)
            if y_planes:
                line = line + row_sum(
                    jnp.where(row_c == r + 1, y_c, 0.0) + jnp.where(row_s == r + 1, y_s, 0.0)
                )
            tile = tile + jnp.where(sub8 == r + 1, line, 0.0)
        return tile

    def assemble(own, kind):
        tiles = {step: rcv[kind, i] for i, step in enumerate(AROUND)}
        tiles[0, 0] = own
        columns = [
            tiles[0, dj]
            + pltpu.roll(jnp.where(sub8 < 4, tiles[1, dj], tiles[-1, dj]), 4, axis=0)
            for dj in (-1, 0, 1)
        ]
        return (
            columns[1]
            + jnp.where(low_lane, pltpu.roll(columns[0], LANES - 4, axis=1), 0.0)
            + jnp.where(low_lane, 0.0, pltpu.roll(columns[2], 4, axis=1))
        )

    def fields(nodes):
        centre, beside = [], []
        for r in range(6):
            value = lane_sum(jnp.broadcast_to(nodes[r + 1 : r + 2], (32, LANES)) * to_col)
            centre.append(value[:16])
            beside.append(value[16:])
        return centre, beside

    def side_field(nodes):
        centre = jnp.zeros((16, LANES), F32)
        beside = jnp.zeros((16, LANES), F32)
        for r in range(1, 7):
            line = jnp.broadcast_to(nodes[r : r + 1], (16, LANES))
            centre = centre + jnp.where(row_c == r, line, 0.0)
            beside = beside + jnp.where(row_s == r, line, 0.0)
        return centre, beside

    def prolong_row(x, centre, beside):
        rc, rs = rows_of_half(x // 2)
        return (
            bas[0, x] * centre[rc]
            + bas[1, x] * centre[rs]
            + bas[2, x] * beside[rc]
            + bas[3, x] * beside[rs]
        )

    def prolong_x_plane(s, centre, beside):
        rc, rs = (5, 4) if s else (0, 1)
        return (
            bxh[s, 0] * centre[rc]
            + bxh[s, 1] * centre[rs]
            + bxh[s, 2] * beside[rc]
            + bxh[s, 3] * beside[rs]
        )

    def prolong_y_plane(s, nodes):
        centre, beside = side_field(nodes)
        near, far = (5, 6) if s else (2, 1)

        def pick(value, lane):
            return lane_sum(jnp.where(lane16 == lane, value, 0.0))

        return (
            byh[s, 0] * pick(centre, far)
            + byh[s, 1] * pick(beside, far)
            + byh[s, 2] * pick(centre, near)
            + byh[s, 3] * pick(beside, near)
        )

    loads[0].wait()
    on_sides(basis_copy, 1, lambda copy: copy.start())
    for s in range(2):
        for k in range(4):
            bys[s, k] = pack_rows(lambda x: bas[k, x, 15 * s : 15 * s + 1, :])
    on_sides(basis_copy, 0, lambda copy: copy.start())
    loads[1].wait()
    own_part = restrict(lambda x: src[x], (), ())
    snd[1] = own_part
    send_tile(1)

    for i in range(4, 13):
        loads[i].wait()
    cell = fcell[...]
    cell_row = cell // CZ
    cell_z = lax.rem(cell, CZ)
    live = (iota((1, FS), 1) < cnt[...]).astype(F32)
    couple = live * flink[...]
    frac_diag = facc[...] + couple + ftrans[0:1] + ftrans[1:2]
    frac_step = OMEGA * live / frac_diag
    for i in range(4):
        zhot[64 * i : 64 * i + 64] = (iota((64, FS), 0) + 64 * i == cell_z).astype(F32).astype(BF16)

    def gather(plane):
        total = jnp.zeros((1, FS), F32)
        for i in range(4):
            high, low = split(plane(i))
            found = dot(high, zhot[...], 0) + dot(low, zhot[...], 0)
            total = total + row_sum(jnp.where(iota((64, FS), 0) + 64 * i == cell_row, found, 0.0))
        return total

    def scatter(values, put):
        for i in range(4):
            high, low = split(jnp.where(iota((64, FS), 0) + 64 * i == cell_row, values, 0.0))
            found = dot(high, zhot[...], 1) + dot(low, zhot[...], 1)
            put(i, found.reshape(4, CY, CZ))

    def put_diag(i, found):
        for j in range(4):
            x = 4 * i + j
            total = found[j] + acc[x]
            for d in range(6):
                total = total + fac[d, x]
            acc[x] = total
            wgt[x] = OMEGA / total

    scatter(couple, put_diag)
    lane_z = iota((16, CZ), 1)
    for x in range(16):
        fac[4, x] = jnp.where(lane_z == CZ - 1, 0.0, fac[4, x])
        fac[5, x] = jnp.where(lane_z == 0, 0.0, fac[5, x])
    edge_face = [
        pack_rows(lambda x: fac[3, x, 0:1, :]),
        pack_rows(lambda x: fac[2, x, 15:16, :]),
    ]

    await_tile(0)
    coarse = assemble(own_static, 0)
    in_group = lane8 < 8
    diag = jnp.where(in_group, coarse, 0.0)
    inverse = jnp.where(diag > 0.0, 1.0 / jnp.where(diag > 0.0, diag, 1.0), 0.0)
    ratio = [
        jnp.where(in_group, pltpu.roll(coarse, LANES - 8 * (g + 1), axis=1), 0.0) for g in range(4)
    ]

    def coarse_solve(own, kind):
        await_tile(kind)
        first = assemble(own, kind) * inverse
        return (
            first
            + ratio[0] * pltpu.roll(first, 1, axis=0)
            + ratio[1] * pltpu.roll(first, 7, axis=0)
            + ratio[2] * pltpu.roll(first, 1, axis=1)
            + ratio[3] * pltpu.roll(first, LANES - 1, axis=1)
        )

    def off_diagonal(p, x):
        middle = p[x + 1, 8:24]
        return (
            fac[0, x] * p[x + 2, 8:24]
            + fac[1, x] * p[x, 8:24]
            + fac[2, x] * p[x + 1, 9:25]
            + fac[3, x] * p[x + 1, 7:23]
            + fac[4, x] * pltpu.roll(middle, CZ - 1, axis=1)
            + fac[5, x] * pltpu.roll(middle, 1, axis=1)
        )

    def own_rows(p, i):
        return p[4 * i + 1 : 4 * i + 5, 8:24].reshape(64, CZ)

    nodes = coarse_solve(own_part, 1)
    centre, beside = fields(nodes)
    for x in range(16):
        P0[x + 1, 8:24] = prolong_row(x, centre, beside)
    frac_now = frac_step * (fsrc[...] + couple * gather(lambda i: own_rows(P0, i)))
    for t in range(4):
        fsnd[t : t + 1, :] = frac_now[:, LANES * t : LANES * t + LANES]

    def frac_copy(s, arrival=False):
        slot = s if arrival else 1 - s
        return pltpu.make_async_remote_copy(
            src_ref=fsnd,
            dst_ref=frcv.at[slot],
            send_sem=frac_ssem.at[s],
            recv_sem=frac_rsem.at[slot],
            device_id=next_dev if s else prev_dev,
            device_id_type=MESH,
        )

    def on_owners(act):
        for s, there in enumerate((has_prev, has_next)):

            @pl.when(there)
            def _():
                act(s)

    on_owners(lambda s: frac_copy(s).start())

    on_sides(lambda axis, s: basis_copy(axis, s, True), 1, lambda copy: copy.wait_recv())
    on_sides(lambda axis, s: basis_copy(axis, s, True), 0, lambda copy: copy.wait_recv())

    def set_rims(p, earlier):
        for s in range(2):
            plane = prolong_x_plane(s, centre, beside)
            p[17 if s else 0, 8:24] = plane + pxh[s] if earlier else plane
            plane = prolong_y_plane(s, nodes)
            if earlier:
                plane = plane + pyh[s]
            for x in range(16):
                p[x + 1, 24 if s else 7, :] = plane[x]

    set_rims(P0, False)
    for x in range(16):
        P1[x + 1, 8:24] = KEEP * P0[x + 1, 8:24] + wgt[x] * (src[x] + off_diagonal(P0, x))
    on_sides(edge_copy, 1, lambda copy: copy.start())
    for s in range(2):
        pys[s] = pack_rows(lambda x: P1[x + 1, 8 + 15 * s : 9 + 15 * s, :])
    on_sides(edge_copy, 0, lambda copy: copy.start())

    def put_source(i, found):
        for j in range(4):
            src[4 * i + j] = src[4 * i + j] + found[j]

    scatter(couple * frac_now, put_source)
    own_part = restrict(
        lambda x: src[x] - acc[x] * P1[x + 1, 8:24] + off_diagonal(P1, x),
        (fac[1, 0] * P1[1, 8:24], fac[0, 15] * P1[16, 8:24]),
        (edge_face[0] * pys[0], edge_face[1] * pys[1]),
    )
    snd[2] = own_part
    send_tile(2)

    nodes = coarse_solve(own_part, 2)
    centre, beside = fields(nodes)
    for x in range(16):
        P0[x + 1, 8:24] = P1[x + 1, 8:24] + prolong_row(x, centre, beside)
    on_sides(lambda axis, s: edge_copy(axis, s, True), 1, lambda copy: copy.wait_recv())
    on_sides(lambda axis, s: edge_copy(axis, s, True), 0, lambda copy: copy.wait_recv())
    set_rims(P0, True)
    for x in range(16):
        out_p[x] = KEEP * P0[x + 1, 8:24] + wgt[x] * (src[x] + off_diagonal(P0, x))

    pressure_at = gather(lambda i: own_rows(P0, i))
    on_owners(lambda s: frac_copy(s, True).wait_recv())
    table = jnp.concatenate([frcv[0], fsnd[...], frcv[1], jnp.zeros((4, LANES), F32)], axis=0)
    high, low = split(table)
    peers = jnp.zeros((1, FS), F32)
    for j in range(2):
        local = fpeer[j : j + 1] - (position - 1) * FS
        hot = (iota((LANES, FS), 0) == lax.rem(local, LANES)).astype(F32).astype(BF16)
        found = dot(high, hot, 0) + dot(low, hot, 0)
        peers = peers + ftrans[j : j + 1] * row_sum(
            jnp.where(iota((16, FS), 0) == local // LANES, found, 0.0)
        )
    out_f[...] = frac_now + frac_step * (
        fsrc[...] + couple * pressure_at + peers - frac_diag * frac_now
    )

    for kind in range(3):
        for i in range(8):

            @pl.when(is_there(AROUND[i]))
            def _():
                tile_copy(kind, i).wait_send()

    for axis in range(2):
        on_sides(basis_copy, axis, lambda copy: copy.wait_send())
        on_sides(edge_copy, axis, lambda copy: copy.wait_send())
    on_owners(lambda s: frac_copy(s).wait_send())


def solution(mesh):
    n_blk, n_lay = mesh.shape["blk"], mesh.shape["lay"]

    def local(src, acc, fac, bas, cd, cr, fs, fa, fl, ft, fc, fp, cnt):
        row = lambda v: v.reshape(1, v.shape[0])
        operands = (src, acc, fac, bas, cd, cr, row(fs), row(fa), row(fl), ft, row(fc), fp, row(cnt))
        vmem = pltpu.VMEM
        pressure, fracture = pl.pallas_call(
            lambda *refs: kernel(n_blk, n_lay, *refs),
            out_shape=(
                jax.ShapeDtypeStruct((CX, CY, CZ), F32),
                jax.ShapeDtypeStruct((1, FS), F32),
            ),
            in_specs=[pl.BlockSpec(memory_space=pl.ANY)] * 13,
            out_specs=[pl.BlockSpec(memory_space=vmem)] * 2,
            scratch_shapes=[vmem(v.shape, v.dtype) for v in operands]
            + [
                vmem((CX + 2, 32, CZ), F32),
                vmem((CX + 2, 32, CZ), F32),
                vmem((CX, CY, CZ), F32),
                vmem((CZ, FS), BF16),
                vmem((5, 8, LANES), F32),
                vmem((3, 8, LANES), F32),
                vmem((3, 8, 8, LANES), F32),
                vmem((2, 4, CY, CZ), F32),
                vmem((2, 4, CX, CZ), F32),
                vmem((2, 4, CX, CZ), F32),
                vmem((2, CY, CZ), F32),
                vmem((2, CX, CZ), F32),
                vmem((2, CX, CZ), F32),
                vmem((4, LANES), F32),
                vmem((2, 4, LANES), F32),
                pltpu.SemaphoreType.DMA((13,)),
                pltpu.SemaphoreType.DMA((3, 8)),
                pltpu.SemaphoreType.DMA((3, 8)),
                pltpu.SemaphoreType.DMA((2, 2)),
                pltpu.SemaphoreType.DMA((2, 2)),
                pltpu.SemaphoreType.DMA((2, 2)),
                pltpu.SemaphoreType.DMA((2, 2)),
                pltpu.SemaphoreType.DMA((2,)),
                pltpu.SemaphoreType.DMA((2,)),
            ],
            compiler_params=pltpu.CompilerParams(collective_id=0, has_side_effects=True),
        )(*operands)
        return pressure, fracture.reshape(FS)

    return jax.shard_map(
        local,
        mesh=mesh,
        in_specs=(
            P("lay", "blk", None),
            P("lay", "blk", None),
            P(None, "lay", "blk", None),
            P(None, "lay", "blk", None),
            P("lay", "blk"),
            P(None, "lay", "blk"),
            P(("blk", "lay")),
            P(("blk", "lay")),
            P(("blk", "lay")),
            P(None, ("blk", "lay")),
            P(("blk", "lay")),
            P(None, ("blk", "lay")),
            P(("blk", "lay")),
        ),
        out_specs=(P("lay", "blk", None), P(("blk", "lay"))),
        check_vma=False,
    )
```

```python
import jax
import jax.numpy as jnp
from jax import lax
from jax.experimental import pallas as pl
from jax.experimental.pallas import tpu as pltpu
from jax.sharding import PartitionSpec as P

MESH = pl.DeviceIdType.MESH
F32 = jnp.float32
BF16 = jnp.bfloat16
I32 = jnp.int32

CX = 16
CY = 16
CZ = 256
FS = 512
OMEGA = 0.8
KEEP = 1.0 - OMEGA
LANES = 128

AROUND = ((-1, -1), (-1, 0), (-1, 1), (0, -1), (0, 1), (1, -1), (1, 0), (1, 1))


def iota(shape, dim):
    return lax.broadcasted_iota(I32, shape, dim)


def lane_sum(v):
    return jnp.sum(v, axis=1, keepdims=True)


def row_sum(v):
    return jnp.sum(v, axis=0, keepdims=True)


def fold(v):
    return v[:, :LANES] + v[:, LANES:]


def split(v):
    high = v.astype(BF16)
    return high, (v - high.astype(F32)).astype(BF16)


def dot(a, b, contract_b):
    return lax.dot_general(a, b, (((1,), (contract_b,)), ((), ())), preferred_element_type=F32)


def kernel(
    n_blk,
    n_lay,
    src_h,
    acc_h,
    fac_h,
    bas_h,
    cd_h,
    cr_h,
    fs_h,
    fa_h,
    fl_h,
    ft_h,
    fc_h,
    fp_h,
    cnt_h,
    out_p,
    out_f,
    src,
    acc,
    fac,
    bas,
    cd,
    cr,
    fsrc,
    facc,
    flink,
    ftrans,
    fcell,
    fpeer,
    cnt,
    P0,
    P1,
    wgt,
    zhot,
    chot,
    near,
    ctile,
    snd,
    rcv,
    bxh,
    byh,
    bys,
    pxh,
    pyh,
    pys,
    fsnd,
    frcv,
    load_sem,
    tile_ssem,
    tile_rsem,
    basis_ssem,
    basis_rsem,
    edge_ssem,
    edge_rsem,
    frac_ssem,
    frac_rsem,
):
    b = lax.axis_index("blk")
    l = lax.axis_index("lay")

    def is_there(step):
        i, j = l + step[0], b + step[1]
        return (i >= 0) & (i < n_lay) & (j >= 0) & (j < n_blk)

    def device(step):
        return (b + step[1], l + step[0])

    position = b * n_lay + l
    has_next = position < n_blk * n_lay - 1
    has_prev = position > 0
    next_dev = ((position + 1) // n_lay, lax.rem(position + 1, n_lay))
    prev_dev = ((position - 1) // n_lay, lax.rem(position - 1 + n_lay, n_lay))

    loads = []
    for i, (hbm, vmem) in enumerate(
        (
            (bas_h, bas),
            (src_h, src),
            (cd_h, cd),
            (cr_h, cr),
            (fc_h, fcell),
            (fl_h, flink),
            (fac_h, fac),
            (acc_h, acc),
            (fs_h, fsrc),
            (fa_h, facc),
            (ft_h, ftrans),
            (fp_h, fpeer),
        )
    ):
        copy = pltpu.make_async_copy(hbm, vmem, load_sem.at[i])
        if i < 2:
            copy.start()
        loads.append(copy)

    barrier = pltpu.get_barrier_semaphore()
    count = jnp.int32(0)
    for step in AROUND:
        there = is_there(step)
        count = count + there.astype(I32)

        @pl.when(there)
        def _():
            pl.semaphore_signal(barrier, inc=1, device_id=device(step), device_id_type=MESH)

    for there, dev in ((has_next, next_dev), (has_prev, prev_dev)):
        count = count + there.astype(I32)

        @pl.when(there)
        def _():
            pl.semaphore_signal(barrier, inc=1, device_id=dev, device_id_type=MESH)

    for i in range(2, len(loads)):
        loads[i].start()

    sides = ((3, 4), (1, 6))
    for i, step in enumerate(AROUND):

        @pl.when(jnp.logical_not(is_there(step)))
        def _():
            for kind in range(2):
                rcv[kind, i] = jnp.zeros((8, LANES), F32)

    for s, there in enumerate((has_prev, has_next)):

        @pl.when(jnp.logical_not(there))
        def _():
            frcv[s] = jnp.zeros((4, LANES), F32)

    for s in range(2):
        step_x = AROUND[sides[1][s]]
        step_y = AROUND[sides[0][s]]

        @pl.when(jnp.logical_not(is_there(step_x)))
        def _():
            bxh[s] = jnp.zeros((4, CY, CZ), F32)
            pxh[s] = jnp.zeros((CY, CZ), F32)

        @pl.when(jnp.logical_not(is_there(step_y)))
        def _():
            byh[s] = jnp.zeros((4, CX, CZ), F32)
            pyh[s] = jnp.zeros((CX, CZ), F32)

    loads[2].wait()
    loads[3].wait()
    ctile[...] = jnp.zeros(ctile.shape, F32)
    ctile[0, 0:4, 0:4] = cd[...]
    for g in range(4):
        ctile[g + 1, 0:4, 0:4] = cr[g]
    own_static = jnp.zeros((8, LANES), F32)
    for g in range(5):
        own_static = own_static + pltpu.roll(pltpu.roll(ctile[g], 2, axis=0), 8 * g + 2, axis=1)

    for s in range(2):
        outer = (15 + 8) if s else 8
        P0[:, outer + (1 if s else -1), :] = jnp.zeros((CX + 2, CZ), F32)
        P1[:, outer + (1 if s else -1), :] = jnp.zeros((CX + 2, CZ), F32)
        P1[17 if s else 0] = jnp.zeros((32, CZ), F32)

    def tile_copy(kind, i):
        return pltpu.make_async_remote_copy(
            src_ref=snd.at[kind],
            dst_ref=rcv.at[kind, 7 - i],
            send_sem=tile_ssem.at[kind, i],
            recv_sem=tile_rsem.at[kind, 7 - i],
            device_id=device(AROUND[i]),
            device_id_type=MESH,
        )

    def tile_arrival(kind, i):
        return pltpu.make_async_remote_copy(
            src_ref=snd.at[kind],
            dst_ref=rcv.at[kind, i],
            send_sem=tile_ssem.at[kind, i],
            recv_sem=tile_rsem.at[kind, i],
            device_id=device(AROUND[i]),
            device_id_type=MESH,
        )

    def send_tile(kind):
        for i in range(8):

            @pl.when(is_there(AROUND[i]))
            def _():
                tile_copy(kind, i).start()

    def await_tile(kind):
        for i in range(8):

            @pl.when(is_there(AROUND[i]))
            def _():
                tile_arrival(kind, i).wait_recv()

    def side_copy(source, target, ssem, rsem, axis, s, arrival=False):
        slot = s if arrival else 1 - s
        return pltpu.make_async_remote_copy(
            src_ref=source,
            dst_ref=target.at[slot],
            send_sem=ssem.at[axis, s],
            recv_sem=rsem.at[axis, slot],
            device_id=device(AROUND[sides[axis][s]]),
            device_id_type=MESH,
        )

    def basis_copy(axis, s, arrival=False):
        source = bas.at[:, 15 * s] if axis else bys.at[s]
        return side_copy(source, bxh if axis else byh, basis_ssem, basis_rsem, axis, s, arrival)

    def edge_copy(axis, s, arrival=False):
        source = P1.at[16 if s else 1, 8:24] if axis else pys.at[s]
        return side_copy(source, pxh if axis else pyh, edge_ssem, edge_rsem, axis, s, arrival)

    def on_sides(make, axis, act):
        for s in range(2):

            @pl.when(is_there(AROUND[sides[axis][s]]))
            def _():
                act(make(axis, s))

    q = iota((32, LANES), 0)
    lane32 = iota((32, LANES), 1)
    y = lax.rem(q, 16)
    col = jnp.where(q < 16, y // 4 + 2, jnp.where(lax.rem(y, 4) < 2, y // 4 + 1, y // 4 + 3))
    to_col = (lane32 == col).astype(F32)
    sub8 = iota((8, LANES), 0)
    lane8 = iota((8, LANES), 1)
    low_lane = lax.rem(lane8, 8) < 4
    x16 = iota((16, LANES), 0)
    lane16 = iota((16, LANES), 1)
    row_c = x16 // 4 + 2
    row_s = jnp.where(lax.rem(x16, 4) < 2, x16 // 4 + 1, x16 // 4 + 3)
    x_wide = iota((16, CZ), 0)

    def rows_of_half(h):
        return h // 2 + 1, (h // 2 if h % 2 == 0 else h // 2 + 2)

    def pack_rows(row):
        value = jnp.broadcast_to(row(0), (16, CZ))
        for x in range(1, 16):
            value = jnp.where(x_wide == x, jnp.broadcast_to(row(x), (16, CZ)), value)
        return value

    def restrict(residual_row, x_planes, y_planes):
        centre = [None] * 6
        beside = [None] * 6

        def add(into, r, value):
            into[r] = value if into[r] is None else into[r] + value

        for h in range(8):
            first, second = residual_row(2 * h), residual_row(2 * h + 1)
            rc, rs = rows_of_half(h)
            for k, (into, r) in enumerate(((centre, rc), (centre, rs), (beside, rc), (beside, rs))):
                add(into, r, fold(bas[k, 2 * h] * first + bas[k, 2 * h + 1] * second))
        for s, plane in enumerate(x_planes):
            rc, rs = (5, 4) if s else (0, 1)
            for k, (into, r) in enumerate(((centre, rc), (centre, rs), (beside, rc), (beside, rs))):
                add(into, r, fold(bxh[s, k] * plane))
        tile = jnp.zeros((8, LANES), F32)
        y_c = jnp.zeros((16, LANES), F32)
        y_s = jnp.zeros((16, LANES), F32)
        for s, plane in enumerate(y_planes):
            near, far = (5, 6) if s else (2, 1)
            for k in range(4):
                value = lane_sum(fold(byh[s, k] * plane))
                placed = jnp.where(lane16 == (far if k < 2 else near), value, 0.0)
                if k % 2 == 0:
                    y_c = y_c + placed
                else:
                    y_s = y_s + placed
        for r in range(6):
            value = lane_sum(jnp.concatenate([centre[r], beside[r]], axis=0))
            line = row_sum(value * to_col)
            if y_planes:
                line = line + row_sum(
                    jnp.where(row_c == r + 1, y_c, 0.0) + jnp.where(row_s == r + 1, y_s, 0.0)
                )
            tile = tile + jnp.where(sub8 == r + 1, line, 0.0)
        return tile

    def assemble(own, kind):
        tiles = {step: rcv[kind, i] for i, step in enumerate(AROUND)}
        tiles[0, 0] = own
        columns = [
            tiles[0, dj]
            + pltpu.roll(jnp.where(sub8 < 4, tiles[1, dj], tiles[-1, dj]), 4, axis=0)
            for dj in (-1, 0, 1)
        ]
        return (
            columns[1]
            + jnp.where(low_lane, pltpu.roll(columns[0], LANES - 4, axis=1), 0.0)
            + jnp.where(low_lane, 0.0, pltpu.roll(columns[2], 4, axis=1))
        )

    def fields(nodes):
        centre, beside = [], []
        for r in range(6):
            value = lane_sum(jnp.broadcast_to(nodes[r + 1 : r + 2], (32, LANES)) * to_col)
            centre.append(value[:16])
            beside.append(value[16:])
        return centre, beside

    def side_field(nodes):
        centre = jnp.zeros((16, LANES), F32)
        beside = jnp.zeros((16, LANES), F32)
        for r in range(1, 7):
            line = jnp.broadcast_to(nodes[r : r + 1], (16, LANES))
            centre = centre + jnp.where(row_c == r, line, 0.0)
            beside = beside + jnp.where(row_s == r, line, 0.0)
        return centre, beside

    def prolong_row(x, centre, beside):
        rc, rs = rows_of_half(x // 2)
        return (
            bas[0, x] * centre[rc]
            + bas[1, x] * centre[rs]
            + bas[2, x] * beside[rc]
            + bas[3, x] * beside[rs]
        )

    def prolong_x_plane(s, centre, beside):
        rc, rs = (5, 4) if s else (0, 1)
        return (
            bxh[s, 0] * centre[rc]
            + bxh[s, 1] * centre[rs]
            + bxh[s, 2] * beside[rc]
            + bxh[s, 3] * beside[rs]
        )

    def prolong_y_plane(s, nodes):
        centre, beside = side_field(nodes)
        near, far = (5, 6) if s else (2, 1)

        def pick(value, lane):
            return lane_sum(jnp.where(lane16 == lane, value, 0.0))

        return (
            byh[s, 0] * pick(centre, far)
            + byh[s, 1] * pick(beside, far)
            + byh[s, 2] * pick(centre, near)
            + byh[s, 3] * pick(beside, near)
        )

    loads[0].wait()
    loads[1].wait()
    own_tile = own_static + pltpu.roll(restrict(lambda x: src[x], (), ()), 40, axis=1)
    snd[0] = own_tile
    for s in range(2):
        for k in range(4):
            bys[s, k] = pack_rows(lambda x: bas[k, x, 15 * s : 15 * s + 1, :])
    pl.semaphore_wait(barrier, count)
    send_tile(0)
    on_sides(basis_copy, 0, lambda copy: copy.start())
    on_sides(basis_copy, 1, lambda copy: copy.start())

    for i in range(4, 12):
        loads[i].wait()
    cell = fcell[...]
    cell_row = cell // CZ
    cell_z = lax.rem(cell, CZ)
    live = (iota((1, FS), 1) < cnt_h[0]).astype(F32)
    couple = live * flink[...]
    frac_diag = facc[...] + couple + ftrans[0:1] + ftrans[1:2]
    frac_step = OMEGA * live / frac_diag
    for i in range(4):
        zhot[64 * i : 64 * i + 64] = (iota((64, FS), 0) + 64 * i == cell_z).astype(F32).astype(BF16)

    def gather(plane):
        total = jnp.zeros((1, FS), F32)
        for i in range(4):
            high, low = split(plane(i))
            found = dot(high, zhot[...], 0) + dot(low, zhot[...], 0)
            total = total + row_sum(jnp.where(iota((64, FS), 0) + 64 * i == cell_row, found, 0.0))
        return total

    def scatter(values, put):
        for i in range(4):
            high, low = split(jnp.where(iota((64, FS), 0) + 64 * i == cell_row, values, 0.0))
            found = dot(high, zhot[...], 1) + dot(low, zhot[...], 1)
            put(i, found.reshape(4, CY, CZ))

    slot_x = cell // (CY * CZ)
    slot_y = lax.rem(cell_row, CY)

    def node_of(v):
        return v // 4 + 2, jnp.where(lax.rem(v, 4) < 2, v // 4 + 1, v // 4 + 3)

    slot_rows = node_of(slot_x)
    slot_cols = node_of(slot_y)
    for i in range(2):
        chot[i] = (iota((LANES, FS), 0) == slot_cols[i]).astype(F32).astype(BF16)
    at_slot = [gather(lambda i: bas[k, 4 * i : 4 * i + 4].reshape(64, CZ)) for k in range(4)]
    sub_slot = iota((8, FS), 0)
    for i in range(2):
        near[i] = jnp.where(sub_slot == slot_rows[0], at_slot[2 * i], 0.0) + jnp.where(
            sub_slot == slot_rows[1], at_slot[2 * i + 1], 0.0
        )

    def prolong_at_slots(nodes):
        high, low = split(nodes)
        return row_sum(
            near[0] * (dot(high, chot[0], 0) + dot(low, chot[0], 0))
            + near[1] * (dot(high, chot[1], 0) + dot(low, chot[1], 0))
        )

    def restrict_from_slots(values):
        total = jnp.zeros((8, LANES), F32)
        for i in range(2):
            high, low = split(near[i] * values)
            total = total + dot(high, chot[i], 1) + dot(low, chot[i], 1)
        return total

    def put_diag(i, found):
        for j in range(4):
            x = 4 * i + j
            total = found[j] + acc[x]
            for d in range(6):
                total = total + fac[d, x]
            acc[x] = total
            wgt[x] = OMEGA / total

    scatter(couple, put_diag)
    lane_z = iota((16, CZ), 1)
    for x in range(16):
        fac[4, x] = jnp.where(lane_z == CZ - 1, 0.0, fac[4, x])
        fac[5, x] = jnp.where(lane_z == 0, 0.0, fac[5, x])
    edge_face = [
        pack_rows(lambda x: fac[3, x, 0:1, :]),
        pack_rows(lambda x: fac[2, x, 15:16, :]),
    ]

    in_group = lane8 < 8

    def group(window, g):
        moved = pltpu.roll(window, LANES - 8 * g, axis=1) if g else window
        return jnp.where(in_group, moved, 0.0)

    def coarse_solve(rhs):
        first = rhs * inverse
        return (
            first
            + ratio[0] * pltpu.roll(first, 1, axis=0)
            + ratio[1] * pltpu.roll(first, 7, axis=0)
            + ratio[2] * pltpu.roll(first, 1, axis=1)
            + ratio[3] * pltpu.roll(first, LANES - 1, axis=1)
        )

    def off_diagonal(p, x):
        middle = p[x + 1, 8:24]
        return (
            fac[0, x] * p[x + 2, 8:24]
            + fac[1, x] * p[x, 8:24]
            + fac[2, x] * p[x + 1, 9:25]
            + fac[3, x] * p[x + 1, 7:23]
            + fac[4, x] * pltpu.roll(middle, CZ - 1, axis=1)
            + fac[5, x] * pltpu.roll(middle, 1, axis=1)
        )

    def own_rows(p, i):
        return p[4 * i + 1 : 4 * i + 5, 8:24].reshape(64, CZ)

    await_tile(0)
    window = assemble(own_tile, 0)
    diag = group(window, 0)
    inverse = jnp.where(diag > 0.0, 1.0 / jnp.where(diag > 0.0, diag, 1.0), 0.0)
    ratio = [group(window, g + 1) for g in range(4)]
    nodes = coarse_solve(group(window, 5))
    centre, beside = fields(nodes)
    for x in range(16):
        P0[x + 1, 8:24] = prolong_row(x, centre, beside)
    frac_now = frac_step * (fsrc[...] + couple * prolong_at_slots(nodes))
    for t in range(4):
        fsnd[t : t + 1, :] = frac_now[:, LANES * t : LANES * t + LANES]

    def frac_copy(s, arrival=False):
        slot = s if arrival else 1 - s
        return pltpu.make_async_remote_copy(
            src_ref=fsnd,
            dst_ref=frcv.at[slot],
            send_sem=frac_ssem.at[s],
            recv_sem=frac_rsem.at[slot],
            device_id=next_dev if s else prev_dev,
            device_id_type=MESH,
        )

    def on_owners(act):
        for s, there in enumerate((has_prev, has_next)):

            @pl.when(there)
            def _():
                act(s)

    on_owners(lambda s: frac_copy(s).start())

    on_sides(lambda axis, s: basis_copy(axis, s, True), 1, lambda copy: copy.wait_recv())
    on_sides(lambda axis, s: basis_copy(axis, s, True), 0, lambda copy: copy.wait_recv())

    def set_rims(p, earlier):
        for s in range(2):
            plane = prolong_x_plane(s, centre, beside)
            p[17 if s else 0, 8:24] = plane + pxh[s] if earlier else plane
            plane = prolong_y_plane(s, nodes)
            if earlier:
                plane = plane + pyh[s]
            for x in range(16):
                p[x + 1, 24 if s else 7, :] = plane[x]

    set_rims(P0, False)
    for x in range(16):
        P1[x + 1, 8:24] = KEEP * P0[x + 1, 8:24] + wgt[x] * (src[x] + off_diagonal(P0, x))
    on_sides(edge_copy, 1, lambda copy: copy.start())
    for s in range(2):
        pys[s] = pack_rows(lambda x: P1[x + 1, 8 + 15 * s : 9 + 15 * s, :])
    on_sides(edge_copy, 0, lambda copy: copy.start())

    own_part = restrict_from_slots(couple * frac_now) + restrict(
        lambda x: src[x] - acc[x] * P1[x + 1, 8:24] + off_diagonal(P1, x),
        (fac[1, 0] * P1[1, 8:24], fac[0, 15] * P1[16, 8:24]),
        (edge_face[0] * pys[0], edge_face[1] * pys[1]),
    )
    snd[1] = own_part
    send_tile(1)

    def put_source(i, found):
        for j in range(4):
            src[4 * i + j] = src[4 * i + j] + found[j]

    scatter(couple * frac_now, put_source)
    pressure_at = gather(lambda i: own_rows(P1, i))
    on_owners(lambda s: frac_copy(s, True).wait_recv())
    table = jnp.concatenate([frcv[0], fsnd[...], frcv[1], jnp.zeros((4, LANES), F32)], axis=0)
    high, low = split(table)
    peers = jnp.zeros((1, FS), F32)
    for j in range(2):
        local = fpeer[j : j + 1] - (position - 1) * FS
        hot = (iota((LANES, FS), 0) == lax.rem(local, LANES)).astype(F32).astype(BF16)
        found = dot(high, hot, 0) + dot(low, hot, 0)
        peers = peers + ftrans[j : j + 1] * row_sum(
            jnp.where(iota((16, FS), 0) == local // LANES, found, 0.0)
        )

    await_tile(1)
    nodes = coarse_solve(assemble(own_part, 1))
    centre, beside = fields(nodes)
    for x in range(16):
        P0[x + 1, 8:24] = P1[x + 1, 8:24] + prolong_row(x, centre, beside)
    on_sides(lambda axis, s: edge_copy(axis, s, True), 1, lambda copy: copy.wait_recv())
    on_sides(lambda axis, s: edge_copy(axis, s, True), 0, lambda copy: copy.wait_recv())
    set_rims(P0, True)
    for x in range(16):
        out_p[x] = KEEP * P0[x + 1, 8:24] + wgt[x] * (src[x] + off_diagonal(P0, x))

    out_f[...] = frac_now + frac_step * (
        fsrc[...] + couple * (pressure_at + prolong_at_slots(nodes)) + peers - frac_diag * frac_now
    )

    for kind in range(2):
        for i in range(8):

            @pl.when(is_there(AROUND[i]))
            def _():
                tile_copy(kind, i).wait_send()

    for axis in range(2):
        on_sides(basis_copy, axis, lambda copy: copy.wait_send())
        on_sides(edge_copy, axis, lambda copy: copy.wait_send())
    on_owners(lambda s: frac_copy(s).wait_send())


def solution(mesh):
    n_blk, n_lay = mesh.shape["blk"], mesh.shape["lay"]

    def local(src, acc, fac, bas, cd, cr, fs, fa, fl, ft, fc, fp, cnt):
        row = lambda v: v.reshape(1, v.shape[0])
        operands = (src, acc, fac, bas, cd, cr, row(fs), row(fa), row(fl), ft, row(fc), fp, cnt)
        vmem = pltpu.VMEM
        pressure, fracture = pl.pallas_call(
            lambda *refs: kernel(n_blk, n_lay, *refs),
            out_shape=(
                vmem((CX, CY, CZ), F32),
                vmem((1, FS), F32),
            ),
            in_specs=[pl.BlockSpec(memory_space=pltpu.HBM)] * 12 + [pl.BlockSpec(memory_space=pltpu.SMEM)],
            out_specs=[pl.BlockSpec(memory_space=vmem)] * 2,
            scratch_shapes=[vmem(v.shape, v.dtype) for v in operands[:-1]]
            + [pltpu.SMEM((1,), I32)]
            + [
                vmem((CX + 2, 32, CZ), F32),
                vmem((CX + 2, 32, CZ), F32),
                vmem((CX, CY, CZ), F32),
                vmem((CZ, FS), BF16),
                vmem((2, LANES, FS), BF16),
                vmem((2, 8, FS), F32),
                vmem((5, 8, LANES), F32),
                vmem((2, 8, LANES), F32),
                vmem((2, 8, 8, LANES), F32),
                vmem((2, 4, CY, CZ), F32),
                vmem((2, 4, CX, CZ), F32),
                vmem((2, 4, CX, CZ), F32),
                vmem((2, CY, CZ), F32),
                vmem((2, CX, CZ), F32),
                vmem((2, CX, CZ), F32),
                vmem((4, LANES), F32),
                vmem((2, 4, LANES), F32),
                pltpu.SemaphoreType.DMA((13,)),
                pltpu.SemaphoreType.DMA((2, 8)),
                pltpu.SemaphoreType.DMA((2, 8)),
                pltpu.SemaphoreType.DMA((2, 2)),
                pltpu.SemaphoreType.DMA((2, 2)),
                pltpu.SemaphoreType.DMA((2, 2)),
                pltpu.SemaphoreType.DMA((2, 2)),
                pltpu.SemaphoreType.DMA((2,)),
                pltpu.SemaphoreType.DMA((2,)),
            ],
            compiler_params=pltpu.CompilerParams(collective_id=0, has_side_effects=True),
        )(*operands)
        return pressure, fracture.reshape(FS)

    return jax.shard_map(
        local,
        mesh=mesh,
        in_specs=(
            P("lay", "blk", None),
            P("lay", "blk", None),
            P(None, "lay", "blk", None),
            P(None, "lay", "blk", None),
            P("lay", "blk"),
            P(None, "lay", "blk"),
            P(("blk", "lay")),
            P(("blk", "lay")),
            P(("blk", "lay")),
            P(None, ("blk", "lay")),
            P(("blk", "lay")),
            P(None, ("blk", "lay")),
            P(("blk", "lay")),
        ),
        out_specs=(P("lay", "blk", None), P(("blk", "lay"))),
        check_vma=False,
    )
```

```python
import jax
import jax.numpy as jnp
from jax import lax
from jax.experimental import pallas as pl
from jax.experimental.pallas import tpu as pltpu
from jax.sharding import PartitionSpec as P

MESH = pl.DeviceIdType.MESH
F32 = jnp.float32
BF16 = jnp.bfloat16
I32 = jnp.int32

CX = 16
CY = 16
CZ = 256
FS = 512
OMEGA = 0.8
KEEP = 1.0 - OMEGA
LANES = 128

AROUND = ((-1, -1), (-1, 0), (-1, 1), (0, -1), (0, 1), (1, -1), (1, 0), (1, 1))
ORDER = (2, 7, 4, 0, 5, 3, 1, 6)


def iota(shape, dim):
    return lax.broadcasted_iota(I32, shape, dim)


def lane_sum(v):
    return jnp.sum(v, axis=1, keepdims=True)


def row_sum(v):
    return jnp.sum(v, axis=0, keepdims=True)


def fold(v):
    return v[:, :LANES] + v[:, LANES:]


def split(v):
    high = v.astype(BF16)
    return high, (v - high.astype(F32)).astype(BF16)


def dot(a, b, contract_b):
    return lax.dot_general(a, b, (((1,), (contract_b,)), ((), ())), preferred_element_type=F32)


def kernel(
    n_blk,
    n_lay,
    src_h,
    acc_h,
    fac_h,
    bas_h,
    cd_h,
    cr_h,
    fs_h,
    fa_h,
    fl_h,
    ft_h,
    fc_h,
    fp_h,
    cnt_h,
    out_p,
    out_f,
    src,
    acc,
    fac,
    bas,
    cd,
    cr,
    fsrc,
    facc,
    flink,
    ftrans,
    fcell,
    fpeer,
    cnt,
    P0,
    P1,
    wgt,
    zhot,
    chot,
    near,
    ctile,
    snd,
    rcv,
    bh,
    bys,
    ph,
    pys,
    fsnd,
    frcv,
    load_sem,
    sems,
):
    b = lax.axis_index("blk")
    l = lax.axis_index("lay")

    def is_there(step):
        i, j = l + step[0], b + step[1]
        return (i >= 0) & (i < n_lay) & (j >= 0) & (j < n_blk)

    def device(step):
        return (b + step[1], l + step[0])

    position = b * n_lay + l
    has_next = position < n_blk * n_lay - 1
    has_prev = position > 0
    next_dev = ((position + 1) // n_lay, lax.rem(position + 1, n_lay))
    prev_dev = ((position - 1) // n_lay, lax.rem(position - 1 + n_lay, n_lay))

    n_i = (l > 0).astype(I32) + (l < n_lay - 1).astype(I32)
    n_j = (b > 0).astype(I32) + (b < n_blk - 1).astype(I32)
    n_sides = n_i + n_j
    n_around = n_sides + n_i * n_j
    n_owners = has_prev.astype(I32) + has_next.astype(I32)

    def wait_all(n, most, block, sem):
        for m in range(1, most + 1):

            @pl.when(n == m)
            def _():
                pltpu.make_async_copy(block.at[0:m], block.at[0:m], sem).wait()

    loads = []
    for i, (hbm, vmem) in enumerate(
        (
            (bas_h, bas),
            (src_h, src),
            (cd_h, cd),
            (cr_h, cr),
            (fc_h, fcell),
            (fl_h, flink),
            (fac_h, fac),
            (acc_h, acc),
            (fs_h, fsrc),
            (fa_h, facc),
            (ft_h, ftrans),
            (fp_h, fpeer),
        )
    ):
        copy = pltpu.make_async_copy(hbm, vmem, load_sem.at[i])
        if i < 2:
            copy.start()
        loads.append(copy)

    barrier = pltpu.get_barrier_semaphore()
    count = jnp.int32(0)
    for i in ORDER:
        step = AROUND[i]
        there = is_there(step)
        count = count + there.astype(I32)

        @pl.when(there)
        def _():
            pl.semaphore_signal(barrier, inc=1, device_id=device(step), device_id_type=MESH)

    for there, dev in ((has_next, next_dev), (has_prev, prev_dev)):
        count = count + there.astype(I32)

        @pl.when(there)
        def _():
            pl.semaphore_signal(barrier, inc=1, device_id=dev, device_id_type=MESH)

    for i in range(2, len(loads)):
        loads[i].start()

    sides = ((3, 4), (1, 6))
    for i, step in enumerate(AROUND):

        @pl.when(jnp.logical_not(is_there(step)))
        def _():
            for kind in range(2):
                rcv[kind, i] = jnp.zeros((8, LANES), F32)

    for s, there in enumerate((has_prev, has_next)):

        @pl.when(jnp.logical_not(there))
        def _():
            frcv[s] = jnp.zeros((4, LANES), F32)

    for s in range(2):
        step_x = AROUND[sides[1][s]]
        step_y = AROUND[sides[0][s]]

        @pl.when(jnp.logical_not(is_there(step_x)))
        def _():
            bh[2 + s] = jnp.zeros((4, CY, CZ), F32)
            ph[2 + s] = jnp.zeros((CY, CZ), F32)

        @pl.when(jnp.logical_not(is_there(step_y)))
        def _():
            bh[s] = jnp.zeros((4, CX, CZ), F32)
            ph[s] = jnp.zeros((CX, CZ), F32)

    loads[2].wait()
    loads[3].wait()
    ctile[...] = jnp.zeros(ctile.shape, F32)
    ctile[0, 0:4, 0:4] = cd[...]
    for g in range(4):
        ctile[g + 1, 0:4, 0:4] = cr[g]
    own_static = jnp.zeros((8, LANES), F32)
    for g in range(5):
        own_static = own_static + pltpu.roll(pltpu.roll(ctile[g], 2, axis=0), 8 * g + 2, axis=1)

    for s in range(2):
        outer = (15 + 8) if s else 8
        P0[:, outer + (1 if s else -1), :] = jnp.zeros((CX + 2, CZ), F32)
        P1[:, outer + (1 if s else -1), :] = jnp.zeros((CX + 2, CZ), F32)
        P1[17 if s else 0] = jnp.zeros((32, CZ), F32)

    def tile_copy(kind, i):
        return pltpu.make_async_remote_copy(
            src_ref=snd.at[kind],
            dst_ref=rcv.at[kind, 7 - i],
            send_sem=sems.at[0],
            recv_sem=sems.at[1 + kind],
            device_id=device(AROUND[i]),
            device_id_type=MESH,
        )

    def send_tile(kind):
        for i in ORDER:

            @pl.when(is_there(AROUND[i]))
            def _():
                tile_copy(kind, i).start()

    def await_tile(kind):
        wait_all(n_around, 8, rcv.at[kind], sems.at[1 + kind])

    def side_copy(source, target, ssem, rsem, axis, s):
        return pltpu.make_async_remote_copy(
            src_ref=source,
            dst_ref=target.at[2 * axis + 1 - s],
            send_sem=ssem,
            recv_sem=rsem,
            device_id=device(AROUND[sides[axis][s]]),
            device_id_type=MESH,
        )

    def basis_copy(axis, s):
        source = bas.at[:, 15 * s] if axis else bys.at[s]
        return side_copy(source, bh, sems.at[3], sems.at[4], axis, s)

    def edge_copy(axis, s):
        source = P1.at[16 if s else 1, 8:24] if axis else pys.at[s]
        return side_copy(source, ph, sems.at[3], sems.at[5], axis, s)

    def on_sides(make, axis, act):
        for s in range(2):

            @pl.when(is_there(AROUND[sides[axis][s]]))
            def _():
                act(make(axis, s))

    q = iota((32, LANES), 0)
    lane32 = iota((32, LANES), 1)
    y = lax.rem(q, 16)
    col = jnp.where(q < 16, y // 4 + 2, jnp.where(lax.rem(y, 4) < 2, y // 4 + 1, y // 4 + 3))
    to_col = (lane32 == col).astype(F32)
    sub8 = iota((8, LANES), 0)
    lane8 = iota((8, LANES), 1)
    low_lane = lax.rem(lane8, 8) < 4
    x16 = iota((16, LANES), 0)
    lane16 = iota((16, LANES), 1)
    row_c = x16 // 4 + 2
    row_s = jnp.where(lax.rem(x16, 4) < 2, x16 // 4 + 1, x16 // 4 + 3)
    x_wide = iota((16, CZ), 0)

    def rows_of_half(h):
        return h // 2 + 1, (h // 2 if h % 2 == 0 else h // 2 + 2)

    def pack_rows(row):
        value = jnp.broadcast_to(row(0), (16, CZ))
        for x in range(1, 16):
            value = jnp.where(x_wide == x, jnp.broadcast_to(row(x), (16, CZ)), value)
        return value

    def restrict(residual_row, x_planes, y_planes):
        centre = [None] * 6
        beside = [None] * 6

        def add(into, r, value):
            into[r] = value if into[r] is None else into[r] + value

        for h in range(8):
            first, second = residual_row(2 * h), residual_row(2 * h + 1)
            rc, rs = rows_of_half(h)
            for k, (into, r) in enumerate(((centre, rc), (centre, rs), (beside, rc), (beside, rs))):
                add(into, r, fold(bas[k, 2 * h] * first + bas[k, 2 * h + 1] * second))
        for s, plane in enumerate(x_planes):
            rc, rs = (5, 4) if s else (0, 1)
            for k, (into, r) in enumerate(((centre, rc), (centre, rs), (beside, rc), (beside, rs))):
                add(into, r, fold(bh[2 + s, k] * plane))
        tile = jnp.zeros((8, LANES), F32)
        y_c = jnp.zeros((16, LANES), F32)
        y_s = jnp.zeros((16, LANES), F32)
        for s, plane in enumerate(y_planes):
            near, far = (5, 6) if s else (2, 1)
            for k in range(4):
                value = lane_sum(fold(bh[s, k] * plane))
                placed = jnp.where(lane16 == (far if k < 2 else near), value, 0.0)
                if k % 2 == 0:
                    y_c = y_c + placed
                else:
                    y_s = y_s + placed
        for r in range(6):
            value = lane_sum(jnp.concatenate([centre[r], beside[r]], axis=0))
            line = row_sum(value * to_col)
            if y_planes:
                line = line + row_sum(
                    jnp.where(row_c == r + 1, y_c, 0.0) + jnp.where(row_s == r + 1, y_s, 0.0)
                )
            tile = tile + jnp.where(sub8 == r + 1, line, 0.0)
        return tile

    def assemble(own, kind):
        tiles = {step: rcv[kind, i] for i, step in enumerate(AROUND)}
        tiles[0, 0] = own
        columns = [
            tiles[0, dj]
            + pltpu.roll(jnp.where(sub8 < 4, tiles[1, dj], tiles[-1, dj]), 4, axis=0)
            for dj in (-1, 0, 1)
        ]
        return (
            columns[1]
            + jnp.where(low_lane, pltpu.roll(columns[0], LANES - 4, axis=1), 0.0)
            + jnp.where(low_lane, 0.0, pltpu.roll(columns[2], 4, axis=1))
        )

    def fields(nodes):
        centre, beside = [], []
        for r in range(6):
            value = lane_sum(jnp.broadcast_to(nodes[r + 1 : r + 2], (32, LANES)) * to_col)
            centre.append(value[:16])
            beside.append(value[16:])
        return centre, beside

    def side_field(nodes):
        centre = jnp.zeros((16, LANES), F32)
        beside = jnp.zeros((16, LANES), F32)
        for r in range(1, 7):
            line = jnp.broadcast_to(nodes[r : r + 1], (16, LANES))
            centre = centre + jnp.where(row_c == r, line, 0.0)
            beside = beside + jnp.where(row_s == r, line, 0.0)
        return centre, beside

    def prolong_row(x, centre, beside):
        rc, rs = rows_of_half(x // 2)
        return (
            bas[0, x] * centre[rc]
            + bas[1, x] * centre[rs]
            + bas[2, x] * beside[rc]
            + bas[3, x] * beside[rs]
        )

    def prolong_x_plane(s, centre, beside):
        rc, rs = (5, 4) if s else (0, 1)
        return (
            bh[2 + s, 0] * centre[rc]
            + bh[2 + s, 1] * centre[rs]
            + bh[2 + s, 2] * beside[rc]
            + bh[2 + s, 3] * beside[rs]
        )

    def prolong_y_plane(s, nodes):
        centre, beside = side_field(nodes)
        near, far = (5, 6) if s else (2, 1)

        def pick(value, lane):
            return lane_sum(jnp.where(lane16 == lane, value, 0.0))

        return (
            bh[s, 0] * pick(centre, far)
            + bh[s, 1] * pick(beside, far)
            + bh[s, 2] * pick(centre, near)
            + bh[s, 3] * pick(beside, near)
        )

    loads[0].wait()
    loads[1].wait()
    own_tile = own_static + pltpu.roll(restrict(lambda x: src[x], (), ()), 40, axis=1)
    snd[0] = own_tile
    for s in range(2):
        for k in range(4):
            bys[s, k] = pack_rows(lambda x: bas[k, x, 15 * s : 15 * s + 1, :])
    pl.semaphore_wait(barrier, count)
    send_tile(0)
    on_sides(basis_copy, 0, lambda copy: copy.start())
    on_sides(basis_copy, 1, lambda copy: copy.start())

    for i in range(4, 12):
        loads[i].wait()
    cell = fcell[...]
    cell_row = cell // CZ
    cell_z = lax.rem(cell, CZ)
    live = (iota((1, FS), 1) < cnt_h[0]).astype(F32)
    couple = live * flink[...]
    frac_diag = facc[...] + couple + ftrans[0:1] + ftrans[1:2]
    frac_step = OMEGA * live / frac_diag
    for i in range(4):
        zhot[64 * i : 64 * i + 64] = (iota((64, FS), 0) + 64 * i == cell_z).astype(F32).astype(BF16)

    def gather(plane):
        total = jnp.zeros((1, FS), F32)
        for i in range(4):
            high, low = split(plane(i))
            found = dot(high, zhot[...], 0) + dot(low, zhot[...], 0)
            total = total + row_sum(jnp.where(iota((64, FS), 0) + 64 * i == cell_row, found, 0.0))
        return total

    def scatter(values, put):
        for i in range(4):
            high, low = split(jnp.where(iota((64, FS), 0) + 64 * i == cell_row, values, 0.0))
            found = dot(high, zhot[...], 1) + dot(low, zhot[...], 1)
            put(i, found.reshape(4, CY, CZ))

    slot_x = cell // (CY * CZ)
    slot_y = lax.rem(cell_row, CY)

    def node_of(v):
        return v // 4 + 2, jnp.where(lax.rem(v, 4) < 2, v // 4 + 1, v // 4 + 3)

    slot_rows = node_of(slot_x)
    slot_cols = node_of(slot_y)
    for i in range(2):
        chot[i] = (iota((LANES, FS), 0) == slot_cols[i]).astype(F32).astype(BF16)
    at_slot = [gather(lambda i: bas[k, 4 * i : 4 * i + 4].reshape(64, CZ)) for k in range(4)]
    sub_slot = iota((8, FS), 0)
    for i in range(2):
        near[i] = jnp.where(sub_slot == slot_rows[0], at_slot[2 * i], 0.0) + jnp.where(
            sub_slot == slot_rows[1], at_slot[2 * i + 1], 0.0
        )

    def prolong_at_slots(nodes):
        high, low = split(nodes)
        return row_sum(
            near[0] * (dot(high, chot[0], 0) + dot(low, chot[0], 0))
            + near[1] * (dot(high, chot[1], 0) + dot(low, chot[1], 0))
        )

    def restrict_from_slots(values):
        total = jnp.zeros((8, LANES), F32)
        for i in range(2):
            high, low = split(near[i] * values)
            total = total + dot(high, chot[i], 1) + dot(low, chot[i], 1)
        return total

    def put_diag(i, found):
        for j in range(4):
            x = 4 * i + j
            total = found[j] + acc[x]
            for d in range(6):
                total = total + fac[d, x]
            acc[x] = total
            wgt[x] = OMEGA / total

    scatter(couple, put_diag)
    lane_z = iota((16, CZ), 1)
    for x in range(16):
        fac[4, x] = jnp.where(lane_z == CZ - 1, 0.0, fac[4, x])
        fac[5, x] = jnp.where(lane_z == 0, 0.0, fac[5, x])
    edge_face = [
        pack_rows(lambda x: fac[3, x, 0:1, :]),
        pack_rows(lambda x: fac[2, x, 15:16, :]),
    ]

    in_group = lane8 < 8

    def group(window, g):
        moved = pltpu.roll(window, LANES - 8 * g, axis=1) if g else window
        return jnp.where(in_group, moved, 0.0)

    def coarse_solve(rhs):
        first = rhs * inverse
        return (
            first
            + ratio[0] * pltpu.roll(first, 1, axis=0)
            + ratio[1] * pltpu.roll(first, 7, axis=0)
            + ratio[2] * pltpu.roll(first, 1, axis=1)
            + ratio[3] * pltpu.roll(first, LANES - 1, axis=1)
        )

    def off_diagonal(p, x):
        middle = p[x + 1, 8:24]
        return (
            fac[0, x] * p[x + 2, 8:24]
            + fac[1, x] * p[x, 8:24]
            + fac[2, x] * p[x + 1, 9:25]
            + fac[3, x] * p[x + 1, 7:23]
            + fac[4, x] * pltpu.roll(middle, CZ - 1, axis=1)
            + fac[5, x] * pltpu.roll(middle, 1, axis=1)
        )

    def own_rows(p, i):
        return p[4 * i + 1 : 4 * i + 5, 8:24].reshape(64, CZ)

    await_tile(0)
    window = assemble(own_tile, 0)
    diag = group(window, 0)
    inverse = jnp.where(diag > 0.0, 1.0 / jnp.where(diag > 0.0, diag, 1.0), 0.0)
    ratio = [group(window, g + 1) for g in range(4)]
    nodes = coarse_solve(group(window, 5))
    centre, beside = fields(nodes)
    for x in range(16):
        P0[x + 1, 8:24] = prolong_row(x, centre, beside)
    frac_now = frac_step * (fsrc[...] + couple * prolong_at_slots(nodes))
    for t in range(4):
        fsnd[t : t + 1, :] = frac_now[:, LANES * t : LANES * t + LANES]

    def frac_copy(s):
        return pltpu.make_async_remote_copy(
            src_ref=fsnd,
            dst_ref=frcv.at[1 - s],
            send_sem=sems.at[6],
            recv_sem=sems.at[7],
            device_id=next_dev if s else prev_dev,
            device_id_type=MESH,
        )

    def on_owners(act):
        for s, there in enumerate((has_prev, has_next)):

            @pl.when(there)
            def _():
                act(s)

    on_owners(lambda s: frac_copy(s).start())

    wait_all(n_sides, 4, bh, sems.at[4])

    def set_rims(p, earlier):
        for s in range(2):
            plane = prolong_x_plane(s, centre, beside)
            p[17 if s else 0, 8:24] = plane + ph[2 + s] if earlier else plane
            plane = prolong_y_plane(s, nodes)
            if earlier:
                plane = plane + ph[s]
            for x in range(16):
                p[x + 1, 24 if s else 7, :] = plane[x]

    set_rims(P0, False)
    for x in range(16):
        P1[x + 1, 8:24] = KEEP * P0[x + 1, 8:24] + wgt[x] * (src[x] + off_diagonal(P0, x))
    wait_all(n_sides, 4, bh, sems.at[3])
    on_sides(edge_copy, 1, lambda copy: copy.start())
    for s in range(2):
        pys[s] = pack_rows(lambda x: P1[x + 1, 8 + 15 * s : 9 + 15 * s, :])
    on_sides(edge_copy, 0, lambda copy: copy.start())

    own_part = restrict_from_slots(couple * frac_now) + restrict(
        lambda x: src[x] - acc[x] * P1[x + 1, 8:24] + off_diagonal(P1, x),
        (fac[1, 0] * P1[1, 8:24], fac[0, 15] * P1[16, 8:24]),
        (edge_face[0] * pys[0], edge_face[1] * pys[1]),
    )
    snd[1] = own_part
    wait_all(n_around, 8, rcv.at[0], sems.at[0])
    send_tile(1)

    def put_source(i, found):
        for j in range(4):
            src[4 * i + j] = src[4 * i + j] + found[j]

    scatter(couple * frac_now, put_source)
    pressure_at = gather(lambda i: own_rows(P1, i))
    wait_all(n_owners, 2, frcv, sems.at[7])
    table = jnp.concatenate([frcv[0], fsnd[...], frcv[1], jnp.zeros((4, LANES), F32)], axis=0)
    high, low = split(table)
    peers = jnp.zeros((1, FS), F32)
    for j in range(2):
        local = fpeer[j : j + 1] - (position - 1) * FS
        hot = (iota((LANES, FS), 0) == lax.rem(local, LANES)).astype(F32).astype(BF16)
        found = dot(high, hot, 0) + dot(low, hot, 0)
        peers = peers + ftrans[j : j + 1] * row_sum(
            jnp.where(iota((16, FS), 0) == local // LANES, found, 0.0)
        )

    await_tile(1)
    nodes = coarse_solve(assemble(own_part, 1))
    centre, beside = fields(nodes)
    for x in range(16):
        P0[x + 1, 8:24] = P1[x + 1, 8:24] + prolong_row(x, centre, beside)
    wait_all(n_sides, 4, ph, sems.at[5])
    set_rims(P0, True)
    for x in range(16):
        out_p[x] = KEEP * P0[x + 1, 8:24] + wgt[x] * (src[x] + off_diagonal(P0, x))

    out_f[...] = frac_now + frac_step * (
        fsrc[...] + couple * (pressure_at + prolong_at_slots(nodes)) + peers - frac_diag * frac_now
    )

    wait_all(n_around, 8, rcv.at[1], sems.at[0])
    wait_all(n_sides, 4, ph, sems.at[3])
    wait_all(n_owners, 2, frcv, sems.at[6])


def store(p_v, f_v, p_h, f_h, sem):
    copies = [
        pltpu.make_async_copy(p_v, p_h, sem.at[0]),
        pltpu.make_async_copy(f_v, f_h, sem.at[1]),
    ]
    for copy in copies:
        copy.start()
    for copy in copies:
        copy.wait()


def solution(mesh):
    n_blk, n_lay = mesh.shape["blk"], mesh.shape["lay"]

    def local(src, acc, fac, bas, cd, cr, fs, fa, fl, ft, fc, fp, cnt):
        row = lambda v: v.reshape(1, v.shape[0])
        operands = (src, acc, fac, bas, cd, cr, row(fs), row(fa), row(fl), ft, row(fc), fp, cnt)
        vmem = pltpu.VMEM
        pressure, fracture = pl.pallas_call(
            lambda *refs: kernel(n_blk, n_lay, *refs),
            out_shape=(
                vmem((CX, CY, CZ), F32),
                vmem((1, FS), F32),
            ),
            in_specs=[pl.BlockSpec(memory_space=pltpu.HBM)] * 12 + [pl.BlockSpec(memory_space=pltpu.SMEM)],
            out_specs=[pl.BlockSpec(memory_space=vmem)] * 2,
            scratch_shapes=[vmem(v.shape, v.dtype) for v in operands[:-1]]
            + [pltpu.SMEM((1,), I32)]
            + [
                vmem((CX + 2, 32, CZ), F32),
                vmem((CX + 2, 32, CZ), F32),
                vmem((CX, CY, CZ), F32),
                vmem((CZ, FS), BF16),
                vmem((2, LANES, FS), BF16),
                vmem((2, 8, FS), F32),
                vmem((5, 8, LANES), F32),
                vmem((2, 8, LANES), F32),
                vmem((2, 8, 8, LANES), F32),
                vmem((4, 4, CX, CZ), F32),
                vmem((2, 4, CX, CZ), F32),
                vmem((4, CX, CZ), F32),
                vmem((2, CX, CZ), F32),
                vmem((4, LANES), F32),
                vmem((2, 4, LANES), F32),
                pltpu.SemaphoreType.DMA((12,)),
                pltpu.SemaphoreType.DMA((8,)),
            ],
            compiler_params=pltpu.CompilerParams(collective_id=0, has_side_effects=True),
        )(*operands)
        pressure, fracture = pl.pallas_call(
            store,
            out_shape=(
                jax.ShapeDtypeStruct((CX, CY, CZ), F32),
                jax.ShapeDtypeStruct((1, FS), F32),
            ),
            in_specs=[pl.BlockSpec(memory_space=vmem)] * 2,
            out_specs=[pl.BlockSpec(memory_space=pltpu.HBM)] * 2,
            scratch_shapes=[pltpu.SemaphoreType.DMA((2,))],
        )(
            pltpu.with_memory_space_constraint(pressure, vmem),
            pltpu.with_memory_space_constraint(fracture, vmem),
        )
        return pressure, fracture.reshape(FS)

    return jax.shard_map(
        local,
        mesh=mesh,
        in_specs=(
            P("lay", "blk", None),
            P("lay", "blk", None),
            P(None, "lay", "blk", None),
            P(None, "lay", "blk", None),
            P("lay", "blk"),
            P(None, "lay", "blk"),
            P(("blk", "lay")),
            P(("blk", "lay")),
            P(("blk", "lay")),
            P(None, ("blk", "lay")),
            P(("blk", "lay")),
            P(None, ("blk", "lay")),
            P(("blk", "lay")),
        ),
        out_specs=(P("lay", "blk", None), P(("blk", "lay"))),
        check_vma=False,
    )
```

```python
import jax
import jax.numpy as jnp
from jax import lax
from jax.experimental import pallas as pl
from jax.experimental.pallas import tpu as pltpu
from jax.sharding import PartitionSpec as P

MESH = pl.DeviceIdType.MESH
F32 = jnp.float32
BF16 = jnp.bfloat16
I32 = jnp.int32

CX = 16
CY = 16
CZ = 256
FS = 512
OMEGA = 0.8
KEEP = 1.0 - OMEGA
LANES = 128
ROW = 8

AROUND = ((-1, -1), (-1, 0), (-1, 1), (0, -1), (0, 1), (1, -1), (1, 0), (1, 1))
ORDER = (2, 7, 4, 0, 5, 3, 1, 6)


def iota(shape, dim):
    return lax.broadcasted_iota(I32, shape, dim)


def lane_sum(v):
    return jnp.sum(v, axis=1, keepdims=True)


def row_sum(v):
    return jnp.sum(v, axis=0, keepdims=True)


def fold(v):
    return v[:, :LANES] + v[:, LANES:]


def split(v):
    high = v.astype(BF16)
    return high, (v - high.astype(F32)).astype(BF16)


def dot(a, b, contract_b):
    return lax.dot_general(a, b, (((1,), (contract_b,)), ((), ())), preferred_element_type=F32)


def kernel(
    n_blk,
    n_lay,
    src_h,
    acc_h,
    fac_h,
    bas_h,
    cd_h,
    cr_h,
    fs_h,
    fa_h,
    fl_h,
    ft_h,
    fc_h,
    fp_h,
    cnt_h,
    out_p,
    out_f,
    src,
    acc,
    fac,
    bas,
    cd,
    cr,
    fsrc,
    facc,
    flink,
    ftrans,
    fcell,
    fpeer,
    cnt,
    P0,
    P1,
    wgt,
    zhot,
    chot,
    near,
    ctile,
    snd,
    rcv,
    bh,
    bys,
    ph,
    pys,
    fsnd,
    frcv,
    fpass,
    load_sem,
    sems,
):
    b = lax.axis_index("blk")
    l = lax.axis_index("lay")

    def is_there(step):
        i, j = l + step[0], b + step[1]
        return (i >= 0) & (i < n_lay) & (j >= 0) & (j < n_blk)

    def device(step):
        return (b + step[1], l + step[0])

    position = b * n_lay + l
    has_next = position < n_blk * n_lay - 1
    has_prev = position > 0
    next_dev = ((position + 1) // n_lay, lax.rem(position + 1, n_lay))
    prev_dev = ((position - 1) // n_lay, lax.rem(position - 1 + n_lay, n_lay))

    first = (lax.rem(b, ROW) == 0) & has_prev & (b > 0)
    passes = first & (l == n_lay - 1)
    asks = first & (l == 0)
    sends_prev = has_prev & jnp.logical_not(asks)
    from_next = has_next & jnp.logical_not((lax.rem(b, ROW) == ROW - 1) & (l == n_lay - 1))

    n_i = (l > 0).astype(I32) + (l < n_lay - 1).astype(I32)
    n_j = (b > 0).astype(I32) + (b < n_blk - 1).astype(I32)
    n_sides = n_i + n_j
    n_around = n_sides + n_i * n_j
    n_owners = has_prev.astype(I32) + has_next.astype(I32)

    def wait_all(n, most, block, sem):
        for m in range(1, most + 1):

            @pl.when(n == m)
            def _():
                pltpu.make_async_copy(block.at[0:m], block.at[0:m], sem).wait()

    loads = []
    for i, (hbm, vmem) in enumerate(
        (
            (bas_h, bas),
            (src_h, src),
            (cd_h, cd),
            (cr_h, cr),
            (fc_h, fcell),
            (fl_h, flink),
            (fac_h, fac),
            (acc_h, acc),
            (fs_h, fsrc),
            (fa_h, facc),
            (ft_h, ftrans),
            (fp_h, fpeer),
        )
    ):
        copy = pltpu.make_async_copy(hbm, vmem, load_sem.at[i])
        if i < 2:
            copy.start()
        loads.append(copy)

    barrier = pltpu.get_barrier_semaphore()
    count = jnp.int32(0)
    for i in ORDER:
        step = AROUND[i]
        there = is_there(step)
        count = count + there.astype(I32)

        @pl.when(there)
        def _():
            pl.semaphore_signal(barrier, inc=1, device_id=device(step), device_id_type=MESH)

    for there in (has_next, sends_prev, asks):
        count = count + there.astype(I32)
    for there, dev in ((from_next, next_dev), (has_prev, prev_dev), (passes, (b, 0))):

        @pl.when(there)
        def _():
            pl.semaphore_signal(barrier, inc=1, device_id=dev, device_id_type=MESH)

    for i in range(2, len(loads)):
        loads[i].start()

    sides = ((3, 4), (1, 6))
    for i, step in enumerate(AROUND):

        @pl.when(jnp.logical_not(is_there(step)))
        def _():
            for kind in range(2):
                rcv[kind, i] = jnp.zeros((8, LANES), F32)

    for s, there in enumerate((has_prev, has_next)):

        @pl.when(jnp.logical_not(there))
        def _():
            frcv[s] = jnp.zeros((4, LANES), F32)

    for s in range(2):
        step_x = AROUND[sides[1][s]]
        step_y = AROUND[sides[0][s]]

        @pl.when(jnp.logical_not(is_there(step_x)))
        def _():
            bh[2 + s] = jnp.zeros((4, CY, CZ), F32)
            ph[2 + s] = jnp.zeros((CY, CZ), F32)

        @pl.when(jnp.logical_not(is_there(step_y)))
        def _():
            bh[s] = jnp.zeros((4, CX, CZ), F32)
            ph[s] = jnp.zeros((CX, CZ), F32)

    loads[2].wait()
    loads[3].wait()
    ctile[...] = jnp.zeros(ctile.shape, F32)
    ctile[0, 0:4, 0:4] = cd[...]
    for g in range(4):
        ctile[g + 1, 0:4, 0:4] = cr[g]
    own_static = jnp.zeros((8, LANES), F32)
    for g in range(5):
        own_static = own_static + pltpu.roll(pltpu.roll(ctile[g], 2, axis=0), 8 * g + 2, axis=1)

    for s in range(2):
        outer = (15 + 8) if s else 8
        P0[:, outer + (1 if s else -1), :] = jnp.zeros((CX + 2, CZ), F32)
        P1[:, outer + (1 if s else -1), :] = jnp.zeros((CX + 2, CZ), F32)
        P1[17 if s else 0] = jnp.zeros((32, CZ), F32)

    def tile_copy(kind, i):
        return pltpu.make_async_remote_copy(
            src_ref=snd.at[kind],
            dst_ref=rcv.at[kind, 7 - i],
            send_sem=sems.at[0],
            recv_sem=sems.at[1 + kind],
            device_id=device(AROUND[i]),
            device_id_type=MESH,
        )

    def send_tile(kind):
        for i in ORDER:

            @pl.when(is_there(AROUND[i]))
            def _():
                tile_copy(kind, i).start()

    def await_tile(kind):
        wait_all(n_around, 8, rcv.at[kind], sems.at[1 + kind])

    def side_copy(source, target, ssem, rsem, axis, s):
        return pltpu.make_async_remote_copy(
            src_ref=source,
            dst_ref=target.at[2 * axis + 1 - s],
            send_sem=ssem,
            recv_sem=rsem,
            device_id=device(AROUND[sides[axis][s]]),
            device_id_type=MESH,
        )

    def basis_copy(axis, s):
        source = bas.at[:, 15 * s] if axis else bys.at[s]
        return side_copy(source, bh, sems.at[3], sems.at[4 if axis else 8], axis, s)

    def edge_copy(axis, s):
        source = P1.at[16 if s else 1, 8:24] if axis else pys.at[s]
        return side_copy(source, ph, sems.at[3], sems.at[5], axis, s)

    def on_sides(make, axis, act):
        for s in range(2):

            @pl.when(is_there(AROUND[sides[axis][s]]))
            def _():
                act(make(axis, s))

    q = iota((32, LANES), 0)
    lane32 = iota((32, LANES), 1)
    y = lax.rem(q, 16)
    col = jnp.where(q < 16, y // 4 + 2, jnp.where(lax.rem(y, 4) < 2, y // 4 + 1, y // 4 + 3))
    to_col = (lane32 == col).astype(F32)
    sub8 = iota((8, LANES), 0)
    lane8 = iota((8, LANES), 1)
    low_lane = lax.rem(lane8, 8) < 4
    x16 = iota((16, LANES), 0)
    lane16 = iota((16, LANES), 1)
    row_c = x16 // 4 + 2
    row_s = jnp.where(lax.rem(x16, 4) < 2, x16 // 4 + 1, x16 // 4 + 3)
    x_wide = iota((16, CZ), 0)

    def rows_of_half(h):
        return h // 2 + 1, (h // 2 if h % 2 == 0 else h // 2 + 2)

    def pack_rows(row):
        value = jnp.broadcast_to(row(0), (16, CZ))
        for x in range(1, 16):
            value = jnp.where(x_wide == x, jnp.broadcast_to(row(x), (16, CZ)), value)
        return value

    def restrict(residual_row, x_planes, y_planes):
        centre = [None] * 6
        beside = [None] * 6

        def add(into, r, value):
            into[r] = value if into[r] is None else into[r] + value

        for h in range(8):
            first, second = residual_row(2 * h), residual_row(2 * h + 1)
            rc, rs = rows_of_half(h)
            for k, (into, r) in enumerate(((centre, rc), (centre, rs), (beside, rc), (beside, rs))):
                add(into, r, fold(bas[k, 2 * h] * first + bas[k, 2 * h + 1] * second))
        for s, plane in enumerate(x_planes):
            rc, rs = (5, 4) if s else (0, 1)
            for k, (into, r) in enumerate(((centre, rc), (centre, rs), (beside, rc), (beside, rs))):
                add(into, r, fold(bh[2 + s, k] * plane))
        tile = jnp.zeros((8, LANES), F32)
        y_c = jnp.zeros((16, LANES), F32)
        y_s = jnp.zeros((16, LANES), F32)
        for s, plane in enumerate(y_planes):
            near, far = (5, 6) if s else (2, 1)
            for k in range(4):
                value = lane_sum(fold(bh[s, k] * plane))
                placed = jnp.where(lane16 == (far if k < 2 else near), value, 0.0)
                if k % 2 == 0:
                    y_c = y_c + placed
                else:
                    y_s = y_s + placed
        for r in range(6):
            value = lane_sum(jnp.concatenate([centre[r], beside[r]], axis=0))
            line = row_sum(value * to_col)
            if y_planes:
                line = line + row_sum(
                    jnp.where(row_c == r + 1, y_c, 0.0) + jnp.where(row_s == r + 1, y_s, 0.0)
                )
            tile = tile + jnp.where(sub8 == r + 1, line, 0.0)
        return tile

    def assemble(own, kind):
        tiles = {step: rcv[kind, i] for i, step in enumerate(AROUND)}
        tiles[0, 0] = own
        columns = [
            tiles[0, dj]
            + pltpu.roll(jnp.where(sub8 < 4, tiles[1, dj], tiles[-1, dj]), 4, axis=0)
            for dj in (-1, 0, 1)
        ]
        return (
            columns[1]
            + jnp.where(low_lane, pltpu.roll(columns[0], LANES - 4, axis=1), 0.0)
            + jnp.where(low_lane, 0.0, pltpu.roll(columns[2], 4, axis=1))
        )

    def fields(nodes):
        centre, beside = [], []
        for r in range(6):
            value = lane_sum(jnp.broadcast_to(nodes[r + 1 : r + 2], (32, LANES)) * to_col)
            centre.append(value[:16])
            beside.append(value[16:])
        return centre, beside

    def side_field(nodes):
        centre = jnp.zeros((16, LANES), F32)
        beside = jnp.zeros((16, LANES), F32)
        for r in range(1, 7):
            line = jnp.broadcast_to(nodes[r : r + 1], (16, LANES))
            centre = centre + jnp.where(row_c == r, line, 0.0)
            beside = beside + jnp.where(row_s == r, line, 0.0)
        return centre, beside

    def prolong_row(x, centre, beside):
        rc, rs = rows_of_half(x // 2)
        return (
            bas[0, x] * centre[rc]
            + bas[1, x] * centre[rs]
            + bas[2, x] * beside[rc]
            + bas[3, x] * beside[rs]
        )

    def prolong_x_plane(s, centre, beside):
        rc, rs = (5, 4) if s else (0, 1)
        return (
            bh[2 + s, 0] * centre[rc]
            + bh[2 + s, 1] * centre[rs]
            + bh[2 + s, 2] * beside[rc]
            + bh[2 + s, 3] * beside[rs]
        )

    def prolong_y_plane(s, nodes):
        centre, beside = side_field(nodes)
        near, far = (5, 6) if s else (2, 1)

        def pick(value, lane):
            return lane_sum(jnp.where(lane16 == lane, value, 0.0))

        return (
            bh[s, 0] * pick(centre, far)
            + bh[s, 1] * pick(beside, far)
            + bh[s, 2] * pick(centre, near)
            + bh[s, 3] * pick(beside, near)
        )

    loads[0].wait()
    loads[1].wait()
    own_tile = own_static + pltpu.roll(restrict(lambda x: src[x], (), ()), 40, axis=1)
    snd[0] = own_tile
    for s in range(2):
        for k in range(4):
            bys[s, k] = pack_rows(lambda x: bas[k, x, 15 * s : 15 * s + 1, :])
    pl.semaphore_wait(barrier, count)
    send_tile(0)
    def send_y_basis(core):
        for s in range(2):

            @pl.when(is_there(AROUND[sides[0][s]]) & (lax.rem(l, 2) == core))
            def _():
                basis_copy(0, s).start()

    send_y_basis(0)
    on_sides(basis_copy, 1, lambda copy: copy.start())

    for i in range(4, 12):
        loads[i].wait()
    cell = fcell[...]
    cell_row = cell // CZ
    cell_z = lax.rem(cell, CZ)
    live = (iota((1, FS), 1) < cnt_h[0]).astype(F32)
    couple = live * flink[...]
    frac_diag = facc[...] + couple + ftrans[0:1] + ftrans[1:2]
    frac_step = OMEGA * live / frac_diag
    for i in range(4):
        zhot[64 * i : 64 * i + 64] = (iota((64, FS), 0) + 64 * i == cell_z).astype(F32).astype(BF16)

    def gather(plane):
        total = jnp.zeros((1, FS), F32)
        for i in range(4):
            high, low = split(plane(i))
            found = dot(high, zhot[...], 0) + dot(low, zhot[...], 0)
            total = total + row_sum(jnp.where(iota((64, FS), 0) + 64 * i == cell_row, found, 0.0))
        return total

    def scatter(values, put):
        for i in range(4):
            high, low = split(jnp.where(iota((64, FS), 0) + 64 * i == cell_row, values, 0.0))
            found = dot(high, zhot[...], 1) + dot(low, zhot[...], 1)
            put(i, found.reshape(4, CY, CZ))

    slot_x = cell // (CY * CZ)
    slot_y = lax.rem(cell_row, CY)

    def node_of(v):
        return v // 4 + 2, jnp.where(lax.rem(v, 4) < 2, v // 4 + 1, v // 4 + 3)

    slot_rows = node_of(slot_x)
    slot_cols = node_of(slot_y)
    for i in range(2):
        chot[i] = (iota((LANES, FS), 0) == slot_cols[i]).astype(F32).astype(BF16)
    at_slot = []
    for k in range(4):
        at_slot.append(gather(lambda i: bas[k, 4 * i : 4 * i + 4].reshape(64, CZ)))
        if k == 1:
            send_y_basis(1)
    sub_slot = iota((8, FS), 0)
    for i in range(2):
        near[i] = jnp.where(sub_slot == slot_rows[0], at_slot[2 * i], 0.0) + jnp.where(
            sub_slot == slot_rows[1], at_slot[2 * i + 1], 0.0
        )

    def prolong_at_slots(nodes):
        high, low = split(nodes)
        return row_sum(
            near[0] * (dot(high, chot[0], 0) + dot(low, chot[0], 0))
            + near[1] * (dot(high, chot[1], 0) + dot(low, chot[1], 0))
        )

    def restrict_from_slots(values):
        total = jnp.zeros((8, LANES), F32)
        for i in range(2):
            high, low = split(near[i] * values)
            total = total + dot(high, chot[i], 1) + dot(low, chot[i], 1)
        return total

    def put_diag(i, found):
        for j in range(4):
            x = 4 * i + j
            total = found[j] + acc[x]
            for d in range(6):
                total = total + fac[d, x]
            acc[x] = total
            wgt[x] = OMEGA / total

    scatter(couple, put_diag)
    lane_z = iota((16, CZ), 1)
    for x in range(16):
        fac[4, x] = jnp.where(lane_z == CZ - 1, 0.0, fac[4, x])
        fac[5, x] = jnp.where(lane_z == 0, 0.0, fac[5, x])
    edge_wgt = [pack_rows(lambda x: wgt[x, 15 * s : 15 * s + 1, :]) for s in range(2)]
    edge_face = [
        pack_rows(lambda x: fac[3, x, 0:1, :]),
        pack_rows(lambda x: fac[2, x, 15:16, :]),
    ]

    in_group = lane8 < 8

    def group(window, g):
        moved = pltpu.roll(window, LANES - 8 * g, axis=1) if g else window
        return jnp.where(in_group, moved, 0.0)

    def coarse_solve(rhs):
        first = rhs * inverse
        return (
            first
            + ratio[0] * pltpu.roll(first, 1, axis=0)
            + ratio[1] * pltpu.roll(first, 7, axis=0)
            + ratio[2] * pltpu.roll(first, 1, axis=1)
            + ratio[3] * pltpu.roll(first, LANES - 1, axis=1)
        )

    def off_diagonal(p, x):
        middle = p[x + 1, 8:24]
        return (
            fac[0, x] * p[x + 2, 8:24]
            + fac[1, x] * p[x, 8:24]
            + fac[2, x] * p[x + 1, 9:25]
            + fac[3, x] * p[x + 1, 7:23]
            + fac[4, x] * pltpu.roll(middle, CZ - 1, axis=1)
            + fac[5, x] * pltpu.roll(middle, 1, axis=1)
        )

    def own_rows(p, i):
        return p[4 * i + 1 : 4 * i + 5, 8:24].reshape(64, CZ)

    await_tile(0)
    window = assemble(own_tile, 0)
    diag = group(window, 0)
    inverse = jnp.where(diag > 0.0, 1.0 / jnp.where(diag > 0.0, diag, 1.0), 0.0)
    ratio = [group(window, g + 1) for g in range(4)]
    nodes = coarse_solve(group(window, 5))
    centre, beside = fields(nodes)
    for x in range(16):
        P0[x + 1, 8:24] = prolong_row(x, centre, beside)
    frac_now = frac_step * (fsrc[...] + couple * prolong_at_slots(nodes))
    for t in range(4):
        fsnd[t : t + 1, :] = frac_now[:, LANES * t : LANES * t + LANES]

    def frac_copy(s):
        return pltpu.make_async_remote_copy(
            src_ref=fsnd,
            dst_ref=frcv.at[1 - s],
            send_sem=sems.at[6],
            recv_sem=sems.at[7],
            device_id=next_dev if s else prev_dev,
            device_id_type=MESH,
        )

    def pass_in():
        return pltpu.make_async_remote_copy(
            src_ref=fsnd,
            dst_ref=fpass,
            send_sem=sems.at[6],
            recv_sem=sems.at[9],
            device_id=(b, n_lay - 1),
            device_id_type=MESH,
        )

    def pass_out():
        return pltpu.make_async_remote_copy(
            src_ref=fpass,
            dst_ref=frcv.at[1],
            send_sem=sems.at[10],
            recv_sem=sems.at[7],
            device_id=(b - 1, l),
            device_id_type=MESH,
        )

    def on_owners(act):
        for s, there in enumerate((sends_prev, has_next)):

            @pl.when(there)
            def _():
                act(s)

    on_owners(lambda s: frac_copy(s).start())

    @pl.when(asks)
    def _():
        pass_in().start()

    wait_all(n_i, 2, bh, sems.at[4])

    def set_x_rims(p, earlier):
        for s in range(2):
            plane = prolong_x_plane(s, centre, beside)
            p[17 if s else 0, 8:24] = plane + ph[2 + s] if earlier else plane

    set_x_rims(P0, False)
    for x in range(16):
        P1[x + 1, 8:24] = KEEP * P0[x + 1, 8:24] + wgt[x] * (src[x] + off_diagonal(P0, x))
    wait_all(n_j, 2, bh, sems.at[8])
    for s in range(2):
        edge = pack_rows(lambda x: P1[x + 1, 8 + 15 * s : 9 + 15 * s, :])
        edge = edge + edge_wgt[s] * (edge_face[s] * prolong_y_plane(s, nodes))
        pys[s] = edge
        for x in range(16):
            P1[x + 1, 8 + 15 * s, :] = edge[x]
    wait_all(n_sides, 4, bh, sems.at[3])
    on_sides(edge_copy, 1, lambda copy: copy.start())
    on_sides(edge_copy, 0, lambda copy: copy.start())

    own_part = restrict_from_slots(couple * frac_now) + restrict(
        lambda x: src[x] - acc[x] * P1[x + 1, 8:24] + off_diagonal(P1, x),
        (fac[1, 0] * P1[1, 8:24], fac[0, 15] * P1[16, 8:24]),
        (edge_face[0] * pys[0], edge_face[1] * pys[1]),
    )
    snd[1] = own_part
    wait_all(n_around, 8, rcv.at[0], sems.at[0])
    send_tile(1)

    def put_source(i, found):
        for j in range(4):
            src[4 * i + j] = src[4 * i + j] + found[j]

    scatter(couple * frac_now, put_source)
    pressure_at = gather(lambda i: own_rows(P1, i))

    @pl.when(passes)
    def _():
        pass_in().wait_recv()
        pass_out().start()

    wait_all(n_owners, 2, frcv, sems.at[7])
    table = jnp.concatenate([frcv[0], fsnd[...], frcv[1], jnp.zeros((4, LANES), F32)], axis=0)
    high, low = split(table)
    peers = jnp.zeros((1, FS), F32)
    for j in range(2):
        local = fpeer[j : j + 1] - (position - 1) * FS
        hot = (iota((LANES, FS), 0) == lax.rem(local, LANES)).astype(F32).astype(BF16)
        found = dot(high, hot, 0) + dot(low, hot, 0)
        peers = peers + ftrans[j : j + 1] * row_sum(
            jnp.where(iota((16, FS), 0) == local // LANES, found, 0.0)
        )

    await_tile(1)
    nodes = coarse_solve(assemble(own_part, 1))
    centre, beside = fields(nodes)
    for x in range(16):
        P0[x + 1, 8:24] = P1[x + 1, 8:24] + prolong_row(x, centre, beside)
    wait_all(n_sides, 4, ph, sems.at[5])
    set_x_rims(P0, True)
    for s in range(2):
        plane = prolong_y_plane(s, nodes) + ph[s]
        for x in range(16):
            P0[x + 1, 24 if s else 7, :] = plane[x]
    for x in range(16):
        out_p[x] = KEEP * P0[x + 1, 8:24] + wgt[x] * (src[x] + off_diagonal(P0, x))

    out_f[...] = frac_now + frac_step * (
        fsrc[...] + couple * (pressure_at + prolong_at_slots(nodes)) + peers - frac_diag * frac_now
    )

    wait_all(n_around, 8, rcv.at[1], sems.at[0])
    wait_all(n_sides, 4, ph, sems.at[3])
    wait_all(n_owners, 2, frcv, sems.at[6])

    @pl.when(passes)
    def _():
        pass_out().wait_send()


def store(p_v, f_v, p_h, f_h, sem):
    copies = [
        pltpu.make_async_copy(p_v, p_h, sem.at[0]),
        pltpu.make_async_copy(f_v, f_h, sem.at[1]),
    ]
    for copy in copies:
        copy.start()
    for copy in copies:
        copy.wait()


def solution(mesh):
    n_blk, n_lay = mesh.shape["blk"], mesh.shape["lay"]

    def local(src, acc, fac, bas, cd, cr, fs, fa, fl, ft, fc, fp, cnt):
        row = lambda v: v.reshape(1, v.shape[0])
        operands = (src, acc, fac, bas, cd, cr, row(fs), row(fa), row(fl), ft, row(fc), fp, cnt)
        vmem = pltpu.VMEM
        pressure, fracture = pl.pallas_call(
            lambda *refs: kernel(n_blk, n_lay, *refs),
            out_shape=(
                vmem((CX, CY, CZ), F32),
                vmem((1, FS), F32),
            ),
            in_specs=[pl.BlockSpec(memory_space=pltpu.HBM)] * 12 + [pl.BlockSpec(memory_space=pltpu.SMEM)],
            out_specs=[pl.BlockSpec(memory_space=vmem)] * 2,
            scratch_shapes=[vmem(v.shape, v.dtype) for v in operands[:-1]]
            + [pltpu.SMEM((1,), I32)]
            + [
                vmem((CX + 2, 32, CZ), F32),
                vmem((CX + 2, 32, CZ), F32),
                vmem((CX, CY, CZ), F32),
                vmem((CZ, FS), BF16),
                vmem((2, LANES, FS), BF16),
                vmem((2, 8, FS), F32),
                vmem((5, 8, LANES), F32),
                vmem((2, 8, LANES), F32),
                vmem((2, 8, 8, LANES), F32),
                vmem((4, 4, CX, CZ), F32),
                vmem((2, 4, CX, CZ), F32),
                vmem((4, CX, CZ), F32),
                vmem((2, CX, CZ), F32),
                vmem((4, LANES), F32),
                vmem((2, 4, LANES), F32),
                vmem((4, LANES), F32),
                pltpu.SemaphoreType.DMA((12,)),
                pltpu.SemaphoreType.DMA((11,)),
            ],
            compiler_params=pltpu.CompilerParams(collective_id=0, has_side_effects=True),
        )(*operands)
        pressure, fracture = pl.pallas_call(
            store,
            out_shape=(
                jax.ShapeDtypeStruct((CX, CY, CZ), F32),
                jax.ShapeDtypeStruct((1, FS), F32),
            ),
            in_specs=[pl.BlockSpec(memory_space=vmem)] * 2,
            out_specs=[pl.BlockSpec(memory_space=pltpu.HBM)] * 2,
            scratch_shapes=[pltpu.SemaphoreType.DMA((2,))],
        )(
            pltpu.with_memory_space_constraint(pressure, vmem),
            pltpu.with_memory_space_constraint(fracture, vmem),
        )
        return pressure, fracture.reshape(FS)

    return jax.shard_map(
        local,
        mesh=mesh,
        in_specs=(
            P("lay", "blk", None),
            P("lay", "blk", None),
            P(None, "lay", "blk", None),
            P(None, "lay", "blk", None),
            P("lay", "blk"),
            P(None, "lay", "blk"),
            P(("blk", "lay")),
            P(("blk", "lay")),
            P(("blk", "lay")),
            P(None, ("blk", "lay")),
            P(("blk", "lay")),
            P(None, ("blk", "lay")),
            P(("blk", "lay")),
        ),
        out_specs=(P("lay", "blk", None), P(("blk", "lay"))),
        check_vma=False,
    )
```

```python
import jax
import jax.numpy as jnp
from jax import lax
from jax.experimental import pallas as pl
from jax.experimental.pallas import tpu as pltpu
from jax.sharding import PartitionSpec as P

MESH = pl.DeviceIdType.MESH
F32 = jnp.float32
BF16 = jnp.bfloat16
I32 = jnp.int32

CX = 16
CY = 16
CZ = 256
FS = 512
OMEGA = 0.8
KEEP = 1.0 - OMEGA
LANES = 128
ROW = 8

AROUND = ((-1, -1), (-1, 0), (-1, 1), (0, -1), (0, 1), (1, -1), (1, 0), (1, 1))
ORDER = (2, 7, 4, 0, 5, 3, 1, 6)


def iota(shape, dim):
    return lax.broadcasted_iota(I32, shape, dim)


def lane_sum(v):
    return jnp.sum(v, axis=1, keepdims=True)


def row_sum(v):
    return jnp.sum(v, axis=0, keepdims=True)


def fold(v):
    return v[:, :LANES] + v[:, LANES:]


def split(v):
    high = v.astype(BF16)
    return high, (v - high.astype(F32)).astype(BF16)


def dot(a, b, contract_b):
    return lax.dot_general(a, b, (((1,), (contract_b,)), ((), ())), preferred_element_type=F32)


def kernel(
    n_blk,
    n_lay,
    src_h,
    acc_h,
    fac_h,
    bas_h,
    cd_h,
    cr_h,
    fs_h,
    fa_h,
    fl_h,
    ft_h,
    fc_h,
    fp_h,
    cnt_h,
    out_p,
    out_f,
    src,
    acc,
    fac,
    bas,
    cd,
    cr,
    fsrc,
    facc,
    flink,
    ftrans,
    fcell,
    fpeer,
    cnt,
    P0,
    P1,
    wgt,
    zhot,
    chot,
    near,
    ctile,
    snd,
    rcv,
    bh,
    bys,
    ph,
    pys,
    fsnd,
    frcv,
    fpass,
    load_sem,
    sems,
):
    b = lax.axis_index("blk")
    l = lax.axis_index("lay")

    def is_there(step):
        i, j = l + step[0], b + step[1]
        return (i >= 0) & (i < n_lay) & (j >= 0) & (j < n_blk)

    def device(step):
        return (b + step[1], l + step[0])

    position = b * n_lay + l
    has_next = position < n_blk * n_lay - 1
    has_prev = position > 0
    next_dev = ((position + 1) // n_lay, lax.rem(position + 1, n_lay))
    prev_dev = ((position - 1) // n_lay, lax.rem(position - 1 + n_lay, n_lay))

    first = (lax.rem(b, ROW) == 0) & has_prev & (b > 0)
    passes = first & (l == n_lay - 1)
    asks = first & (l == 0)
    sends_prev = has_prev & jnp.logical_not(asks)
    from_next = has_next & jnp.logical_not((lax.rem(b, ROW) == ROW - 1) & (l == n_lay - 1))

    n_i = (l > 0).astype(I32) + (l < n_lay - 1).astype(I32)
    n_j = (b > 0).astype(I32) + (b < n_blk - 1).astype(I32)
    n_sides = n_i + n_j
    n_around = n_sides + n_i * n_j
    n_owners = has_prev.astype(I32) + has_next.astype(I32)

    def wait_all(n, most, block, sem):
        for m in range(1, most + 1):

            @pl.when(n == m)
            def _():
                pltpu.make_async_copy(block.at[0:m], block.at[0:m], sem).wait()

    loads = []
    for i, (hbm, vmem) in enumerate(
        (
            (bas_h, bas),
            (src_h, src),
            (cd_h, cd),
            (cr_h, cr),
            (fc_h, fcell),
            (fl_h, flink),
            (fac_h, fac),
            (acc_h, acc),
            (fs_h, fsrc),
            (fa_h, facc),
            (ft_h, ftrans),
            (fp_h, fpeer),
        )
    ):
        copy = pltpu.make_async_copy(hbm, vmem, load_sem.at[i])
        if i < 2:
            copy.start()
        loads.append(copy)

    barrier = pltpu.get_barrier_semaphore()
    count = jnp.int32(0)
    for i in ORDER:
        step = AROUND[i]
        there = is_there(step)
        count = count + there.astype(I32)

        @pl.when(there)
        def _():
            pl.semaphore_signal(barrier, inc=1, device_id=device(step), device_id_type=MESH)

    for there in (has_next, sends_prev, asks):
        count = count + there.astype(I32)
    for there, dev in ((from_next, next_dev), (has_prev, prev_dev), (passes, (b, 0))):

        @pl.when(there)
        def _():
            pl.semaphore_signal(barrier, inc=1, device_id=dev, device_id_type=MESH)

    for i in range(2, len(loads)):
        loads[i].start()

    sides = ((3, 4), (1, 6))
    for i, step in enumerate(AROUND):

        @pl.when(jnp.logical_not(is_there(step)))
        def _():
            for kind in range(2):
                rcv[kind, i] = jnp.zeros((8, LANES), F32)

    for s, there in enumerate((has_prev, has_next)):

        @pl.when(jnp.logical_not(there))
        def _():
            frcv[s] = jnp.zeros((4, LANES), F32)

    for s in range(2):
        step_x = AROUND[sides[1][s]]
        step_y = AROUND[sides[0][s]]

        @pl.when(jnp.logical_not(is_there(step_x)))
        def _():
            bh[2 + s] = jnp.zeros((4, CY, CZ), F32)
            ph[2 + s] = jnp.zeros((CY, CZ), F32)

        @pl.when(jnp.logical_not(is_there(step_y)))
        def _():
            bh[s] = jnp.zeros((4, CX, CZ), F32)
            ph[s] = jnp.zeros((CX, CZ), F32)

    loads[2].wait()
    loads[3].wait()
    ctile[...] = jnp.zeros(ctile.shape, F32)
    ctile[0, 0:4, 0:4] = cd[...]
    for g in range(4):
        ctile[g + 1, 0:4, 0:4] = cr[g]
    own_static = jnp.zeros((8, LANES), F32)
    for g in range(5):
        own_static = own_static + pltpu.roll(pltpu.roll(ctile[g], 2, axis=0), 8 * g + 2, axis=1)

    for s in range(2):
        outer = (15 + 8) if s else 8
        P0[:, outer + (1 if s else -1), :] = jnp.zeros((CX + 2, CZ), F32)
        P1[:, outer + (1 if s else -1), :] = jnp.zeros((CX + 2, CZ), F32)
        P1[17 if s else 0] = jnp.zeros((32, CZ), F32)

    def tile_copy(kind, i):
        return pltpu.make_async_remote_copy(
            src_ref=snd.at[kind],
            dst_ref=rcv.at[kind, 7 - i],
            send_sem=sems.at[0],
            recv_sem=sems.at[1 + kind],
            device_id=device(AROUND[i]),
            device_id_type=MESH,
        )

    def send_tile(kind):
        for i in ORDER:

            @pl.when(is_there(AROUND[i]))
            def _():
                tile_copy(kind, i).start()

    def await_tile(kind):
        wait_all(n_around, 8, rcv.at[kind], sems.at[1 + kind])

    def side_copy(source, target, ssem, rsem, axis, s):
        return pltpu.make_async_remote_copy(
            src_ref=source,
            dst_ref=target.at[2 * axis + 1 - s],
            send_sem=ssem,
            recv_sem=rsem,
            device_id=device(AROUND[sides[axis][s]]),
            device_id_type=MESH,
        )

    def basis_copy(axis, s):
        source = bas.at[:, 15 * s] if axis else bys.at[s]
        return side_copy(source, bh, sems.at[3], sems.at[4 if axis else 8], axis, s)

    def edge_copy(axis, s):
        source = P1.at[16 if s else 1, 8:24] if axis else pys.at[s]
        return side_copy(source, ph, sems.at[3], sems.at[5], axis, s)

    def on_sides(make, axis, act):
        for s in range(2):

            @pl.when(is_there(AROUND[sides[axis][s]]))
            def _():
                act(make(axis, s))

    q = iota((32, LANES), 0)
    lane32 = iota((32, LANES), 1)
    y = lax.rem(q, 16)
    col = jnp.where(q < 16, y // 4 + 2, jnp.where(lax.rem(y, 4) < 2, y // 4 + 1, y // 4 + 3))
    to_col = (lane32 == col).astype(F32)
    sub8 = iota((8, LANES), 0)
    lane8 = iota((8, LANES), 1)
    low_lane = lax.rem(lane8, 8) < 4
    x16 = iota((16, LANES), 0)
    lane16 = iota((16, LANES), 1)
    row_c = x16 // 4 + 2
    row_s = jnp.where(lax.rem(x16, 4) < 2, x16 // 4 + 1, x16 // 4 + 3)
    x_wide = iota((16, CZ), 0)

    def rows_of_half(h):
        return h // 2 + 1, (h // 2 if h % 2 == 0 else h // 2 + 2)

    def pack_rows(row):
        value = jnp.broadcast_to(row(0), (16, CZ))
        for x in range(1, 16):
            value = jnp.where(x_wide == x, jnp.broadcast_to(row(x), (16, CZ)), value)
        return value

    def restrict(residual_row, x_planes, y_planes):
        centre = [None] * 6
        beside = [None] * 6

        def add(into, r, value):
            into[r] = value if into[r] is None else into[r] + value

        for h in range(8):
            first, second = residual_row(2 * h), residual_row(2 * h + 1)
            rc, rs = rows_of_half(h)
            for k, (into, r) in enumerate(((centre, rc), (centre, rs), (beside, rc), (beside, rs))):
                add(into, r, fold(bas[k, 2 * h] * first + bas[k, 2 * h + 1] * second))
        for s, plane in enumerate(x_planes):
            rc, rs = (5, 4) if s else (0, 1)
            for k, (into, r) in enumerate(((centre, rc), (centre, rs), (beside, rc), (beside, rs))):
                add(into, r, fold(bh[2 + s, k] * plane))
        tile = jnp.zeros((8, LANES), F32)
        y_c = jnp.zeros((16, LANES), F32)
        y_s = jnp.zeros((16, LANES), F32)
        for s, plane in enumerate(y_planes):
            near, far = (5, 6) if s else (2, 1)
            for k in range(4):
                value = lane_sum(fold(bh[s, k] * plane))
                placed = jnp.where(lane16 == (far if k < 2 else near), value, 0.0)
                if k % 2 == 0:
                    y_c = y_c + placed
                else:
                    y_s = y_s + placed
        for r in range(6):
            value = lane_sum(jnp.concatenate([centre[r], beside[r]], axis=0))
            line = row_sum(value * to_col)
            if y_planes:
                line = line + row_sum(
                    jnp.where(row_c == r + 1, y_c, 0.0) + jnp.where(row_s == r + 1, y_s, 0.0)
                )
            tile = tile + jnp.where(sub8 == r + 1, line, 0.0)
        return tile

    def assemble(own, kind):
        tiles = {step: rcv[kind, i] for i, step in enumerate(AROUND)}
        tiles[0, 0] = own
        columns = [
            tiles[0, dj]
            + pltpu.roll(jnp.where(sub8 < 4, tiles[1, dj], tiles[-1, dj]), 4, axis=0)
            for dj in (-1, 0, 1)
        ]
        return (
            columns[1]
            + jnp.where(low_lane, pltpu.roll(columns[0], LANES - 4, axis=1), 0.0)
            + jnp.where(low_lane, 0.0, pltpu.roll(columns[2], 4, axis=1))
        )

    def fields(nodes):
        centre, beside = [], []
        for r in range(6):
            value = lane_sum(jnp.broadcast_to(nodes[r + 1 : r + 2], (32, LANES)) * to_col)
            centre.append(value[:16])
            beside.append(value[16:])
        return centre, beside

    def side_field(nodes):
        centre = jnp.zeros((16, LANES), F32)
        beside = jnp.zeros((16, LANES), F32)
        for r in range(1, 7):
            line = jnp.broadcast_to(nodes[r : r + 1], (16, LANES))
            centre = centre + jnp.where(row_c == r, line, 0.0)
            beside = beside + jnp.where(row_s == r, line, 0.0)
        return centre, beside

    def prolong_row(x, centre, beside):
        rc, rs = rows_of_half(x // 2)
        return (
            bas[0, x] * centre[rc]
            + bas[1, x] * centre[rs]
            + bas[2, x] * beside[rc]
            + bas[3, x] * beside[rs]
        )

    def prolong_x_plane(s, centre, beside):
        rc, rs = (5, 4) if s else (0, 1)
        return (
            bh[2 + s, 0] * centre[rc]
            + bh[2 + s, 1] * centre[rs]
            + bh[2 + s, 2] * beside[rc]
            + bh[2 + s, 3] * beside[rs]
        )

    def prolong_y_plane(s, nodes):
        centre, beside = side_field(nodes)
        near, far = (5, 6) if s else (2, 1)

        def pick(value, lane):
            return lane_sum(jnp.where(lane16 == lane, value, 0.0))

        return (
            bh[s, 0] * pick(centre, far)
            + bh[s, 1] * pick(beside, far)
            + bh[s, 2] * pick(centre, near)
            + bh[s, 3] * pick(beside, near)
        )

    loads[0].wait()
    loads[1].wait()
    own_tile = own_static + pltpu.roll(restrict(lambda x: src[x], (), ()), 40, axis=1)
    snd[0] = own_tile
    for s in range(2):
        for k in range(4):
            bys[s, k] = pack_rows(lambda x: bas[k, x, 15 * s : 15 * s + 1, :])
    pl.semaphore_wait(barrier, count)
    send_tile(0)
    def send_y_basis(core):
        for s in range(2):

            @pl.when(is_there(AROUND[sides[0][s]]) & (lax.rem(l, 2) == core))
            def _():
                basis_copy(0, s).start()

    send_y_basis(0)
    on_sides(basis_copy, 1, lambda copy: copy.start())

    for i in range(4, 12):
        loads[i].wait()
    cell = fcell[...]
    cell_row = cell // CZ
    cell_z = lax.rem(cell, CZ)
    live = (iota((1, FS), 1) < cnt_h[0]).astype(F32)
    couple = live * flink[...]
    frac_diag = facc[...] + couple + ftrans[0:1] + ftrans[1:2]
    frac_step = OMEGA * live / frac_diag
    for i in range(4):
        zhot[64 * i : 64 * i + 64] = (iota((64, FS), 0) + 64 * i == cell_z).astype(F32).astype(BF16)

    def gather(plane):
        total = jnp.zeros((1, FS), F32)
        for i in range(4):
            high, low = split(plane(i))
            found = dot(high, zhot[...], 0) + dot(low, zhot[...], 0)
            total = total + row_sum(jnp.where(iota((64, FS), 0) + 64 * i == cell_row, found, 0.0))
        return total

    def scatter(values, put):
        for i in range(4):
            high, low = split(jnp.where(iota((64, FS), 0) + 64 * i == cell_row, values, 0.0))
            found = dot(high, zhot[...], 1) + dot(low, zhot[...], 1)
            put(i, found.reshape(4, CY, CZ))

    slot_x = cell // (CY * CZ)
    slot_y = lax.rem(cell_row, CY)

    def node_of(v):
        return v // 4 + 2, jnp.where(lax.rem(v, 4) < 2, v // 4 + 1, v // 4 + 3)

    slot_rows = node_of(slot_x)
    slot_cols = node_of(slot_y)
    for i in range(2):
        chot[i] = (iota((LANES, FS), 0) == slot_cols[i]).astype(F32).astype(BF16)
    at_slot = []
    for k in range(4):
        at_slot.append(gather(lambda i: bas[k, 4 * i : 4 * i + 4].reshape(64, CZ)))
        if k == 3:
            send_y_basis(1)
    sub_slot = iota((8, FS), 0)
    for i in range(2):
        near[i] = jnp.where(sub_slot == slot_rows[0], at_slot[2 * i], 0.0) + jnp.where(
            sub_slot == slot_rows[1], at_slot[2 * i + 1], 0.0
        )

    def prolong_at_slots(nodes):
        high, low = split(nodes)
        return row_sum(
            near[0] * (dot(high, chot[0], 0) + dot(low, chot[0], 0))
            + near[1] * (dot(high, chot[1], 0) + dot(low, chot[1], 0))
        )

    def restrict_from_slots(values):
        total = jnp.zeros((8, LANES), F32)
        for i in range(2):
            high, low = split(near[i] * values)
            total = total + dot(high, chot[i], 1) + dot(low, chot[i], 1)
        return total

    def put_diag(i, found):
        for j in range(4):
            x = 4 * i + j
            total = found[j] + acc[x]
            for d in range(6):
                total = total + fac[d, x]
            acc[x] = total
            wgt[x] = OMEGA / total

    scatter(couple, put_diag)
    lane_z = iota((16, CZ), 1)
    for x in range(16):
        fac[4, x] = jnp.where(lane_z == CZ - 1, 0.0, fac[4, x])
        fac[5, x] = jnp.where(lane_z == 0, 0.0, fac[5, x])
    edge_wgt = [pack_rows(lambda x: wgt[x, 15 * s : 15 * s + 1, :]) for s in range(2)]
    edge_face = [
        pack_rows(lambda x: fac[3, x, 0:1, :]),
        pack_rows(lambda x: fac[2, x, 15:16, :]),
    ]

    in_group = lane8 < 8

    def group(window, g):
        moved = pltpu.roll(window, LANES - 8 * g, axis=1) if g else window
        return jnp.where(in_group, moved, 0.0)

    def coarse_solve(rhs):
        first = rhs * inverse
        return (
            first
            + ratio[0] * pltpu.roll(first, 1, axis=0)
            + ratio[1] * pltpu.roll(first, 7, axis=0)
            + ratio[2] * pltpu.roll(first, 1, axis=1)
            + ratio[3] * pltpu.roll(first, LANES - 1, axis=1)
        )

    def off_diagonal(p, x):
        middle = p[x + 1, 8:24]
        return (
            fac[0, x] * p[x + 2, 8:24]
            + fac[1, x] * p[x, 8:24]
            + fac[2, x] * p[x + 1, 9:25]
            + fac[3, x] * p[x + 1, 7:23]
            + fac[4, x] * pltpu.roll(middle, CZ - 1, axis=1)
            + fac[5, x] * pltpu.roll(middle, 1, axis=1)
        )

    def own_rows(p, i):
        return p[4 * i + 1 : 4 * i + 5, 8:24].reshape(64, CZ)

    await_tile(0)
    window = assemble(own_tile, 0)
    diag = group(window, 0)
    inverse = jnp.where(diag > 0.0, 1.0 / jnp.where(diag > 0.0, diag, 1.0), 0.0)
    ratio = [group(window, g + 1) for g in range(4)]
    nodes = coarse_solve(group(window, 5))
    centre, beside = fields(nodes)
    for x in range(16):
        P0[x + 1, 8:24] = prolong_row(x, centre, beside)
    frac_now = frac_step * (fsrc[...] + couple * prolong_at_slots(nodes))
    for t in range(4):
        fsnd[t : t + 1, :] = frac_now[:, LANES * t : LANES * t + LANES]

    def frac_copy(s):
        return pltpu.make_async_remote_copy(
            src_ref=fsnd,
            dst_ref=frcv.at[1 - s],
            send_sem=sems.at[6],
            recv_sem=sems.at[7],
            device_id=next_dev if s else prev_dev,
            device_id_type=MESH,
        )

    def pass_in():
        return pltpu.make_async_remote_copy(
            src_ref=fsnd,
            dst_ref=fpass,
            send_sem=sems.at[6],
            recv_sem=sems.at[9],
            device_id=(b, n_lay - 1),
            device_id_type=MESH,
        )

    def pass_out():
        return pltpu.make_async_remote_copy(
            src_ref=fpass,
            dst_ref=frcv.at[1],
            send_sem=sems.at[10],
            recv_sem=sems.at[7],
            device_id=(b - 1, l),
            device_id_type=MESH,
        )

    def on_owners(act):
        for s, there in enumerate((sends_prev, has_next)):

            @pl.when(there)
            def _():
                act(s)

    on_owners(lambda s: frac_copy(s).start())

    @pl.when(asks)
    def _():
        pass_in().start()

    wait_all(n_i, 2, bh, sems.at[4])

    def set_x_rims(p, earlier):
        for s in range(2):
            plane = prolong_x_plane(s, centre, beside)
            p[17 if s else 0, 8:24] = plane + ph[2 + s] if earlier else plane

    set_x_rims(P0, False)
    for x in range(16):
        P1[x + 1, 8:24] = KEEP * P0[x + 1, 8:24] + wgt[x] * (src[x] + off_diagonal(P0, x))
    wait_all(n_j, 2, bh, sems.at[8])
    for s in range(2):
        edge = pack_rows(lambda x: P1[x + 1, 8 + 15 * s : 9 + 15 * s, :])
        edge = edge + edge_wgt[s] * (edge_face[s] * prolong_y_plane(s, nodes))
        pys[s] = edge
        for x in range(16):
            P1[x + 1, 8 + 15 * s, :] = edge[x]
    wait_all(n_sides, 4, bh, sems.at[3])
    own_part = restrict_from_slots(couple * frac_now) + restrict(
        lambda x: src[x] - acc[x] * P1[x + 1, 8:24] + off_diagonal(P1, x),
        (fac[1, 0] * P1[1, 8:24], fac[0, 15] * P1[16, 8:24]),
        (edge_face[0] * pys[0], edge_face[1] * pys[1]),
    )
    snd[1] = own_part
    wait_all(n_around, 8, rcv.at[0], sems.at[0])
    send_tile(1)
    on_sides(edge_copy, 1, lambda copy: copy.start())
    on_sides(edge_copy, 0, lambda copy: copy.start())


    def put_source(i, found):
        for j in range(4):
            src[4 * i + j] = src[4 * i + j] + found[j]

    scatter(couple * frac_now, put_source)
    pressure_at = gather(lambda i: own_rows(P1, i))

    @pl.when(passes)
    def _():
        pass_in().wait_recv()
        pass_out().start()

    wait_all(n_owners, 2, frcv, sems.at[7])
    table = jnp.concatenate([frcv[0], fsnd[...], frcv[1], jnp.zeros((4, LANES), F32)], axis=0)
    high, low = split(table)
    peers = jnp.zeros((1, FS), F32)
    for j in range(2):
        local = fpeer[j : j + 1] - (position - 1) * FS
        hot = (iota((LANES, FS), 0) == lax.rem(local, LANES)).astype(F32).astype(BF16)
        found = dot(high, hot, 0) + dot(low, hot, 0)
        peers = peers + ftrans[j : j + 1] * row_sum(
            jnp.where(iota((16, FS), 0) == local // LANES, found, 0.0)
        )

    await_tile(1)
    nodes = coarse_solve(assemble(own_part, 1))
    centre, beside = fields(nodes)
    for x in range(16):
        P0[x + 1, 8:24] = P1[x + 1, 8:24] + prolong_row(x, centre, beside)
    wait_all(n_sides, 4, ph, sems.at[5])
    set_x_rims(P0, True)
    for s in range(2):
        plane = prolong_y_plane(s, nodes) + ph[s]
        for x in range(16):
            P0[x + 1, 24 if s else 7, :] = plane[x]
    for x in range(16):
        out_p[x] = KEEP * P0[x + 1, 8:24] + wgt[x] * (src[x] + off_diagonal(P0, x))

    out_f[...] = frac_now + frac_step * (
        fsrc[...] + couple * (pressure_at + prolong_at_slots(nodes)) + peers - frac_diag * frac_now
    )

    wait_all(n_around, 8, rcv.at[1], sems.at[0])
    wait_all(n_sides, 4, ph, sems.at[3])
    wait_all(n_owners, 2, frcv, sems.at[6])

    @pl.when(passes)
    def _():
        pass_out().wait_send()


def store(p_v, f_v, p_h, f_h, sem):
    copies = [
        pltpu.make_async_copy(p_v, p_h, sem.at[0]),
        pltpu.make_async_copy(f_v, f_h, sem.at[1]),
    ]
    for copy in copies:
        copy.start()
    for copy in copies:
        copy.wait()


def solution(mesh):
    n_blk, n_lay = mesh.shape["blk"], mesh.shape["lay"]

    def local(src, acc, fac, bas, cd, cr, fs, fa, fl, ft, fc, fp, cnt):
        row = lambda v: v.reshape(1, v.shape[0])
        operands = (src, acc, fac, bas, cd, cr, row(fs), row(fa), row(fl), ft, row(fc), fp, cnt)
        vmem = pltpu.VMEM
        pressure, fracture = pl.pallas_call(
            lambda *refs: kernel(n_blk, n_lay, *refs),
            out_shape=(
                vmem((CX, CY, CZ), F32),
                vmem((1, FS), F32),
            ),
            in_specs=[pl.BlockSpec(memory_space=pltpu.HBM)] * 12 + [pl.BlockSpec(memory_space=pltpu.SMEM)],
            out_specs=[pl.BlockSpec(memory_space=vmem)] * 2,
            scratch_shapes=[vmem(v.shape, v.dtype) for v in operands[:-1]]
            + [pltpu.SMEM((1,), I32)]
            + [
                vmem((CX + 2, 32, CZ), F32),
                vmem((CX + 2, 32, CZ), F32),
                vmem((CX, CY, CZ), F32),
                vmem((CZ, FS), BF16),
                vmem((2, LANES, FS), BF16),
                vmem((2, 8, FS), F32),
                vmem((5, 8, LANES), F32),
                vmem((2, 8, LANES), F32),
                vmem((2, 8, 8, LANES), F32),
                vmem((4, 4, CX, CZ), F32),
                vmem((2, 4, CX, CZ), F32),
                vmem((4, CX, CZ), F32),
                vmem((2, CX, CZ), F32),
                vmem((4, LANES), F32),
                vmem((2, 4, LANES), F32),
                vmem((4, LANES), F32),
                pltpu.SemaphoreType.DMA((12,)),
                pltpu.SemaphoreType.DMA((11,)),
            ],
            compiler_params=pltpu.CompilerParams(collective_id=0, has_side_effects=True),
        )(*operands)
        pressure, fracture = pl.pallas_call(
            store,
            out_shape=(
                jax.ShapeDtypeStruct((CX, CY, CZ), F32),
                jax.ShapeDtypeStruct((1, FS), F32),
            ),
            in_specs=[pl.BlockSpec(memory_space=vmem)] * 2,
            out_specs=[pl.BlockSpec(memory_space=pltpu.HBM)] * 2,
            scratch_shapes=[pltpu.SemaphoreType.DMA((2,))],
        )(
            pltpu.with_memory_space_constraint(pressure, vmem),
            pltpu.with_memory_space_constraint(fracture, vmem),
        )
        return pressure, fracture.reshape(FS)

    return jax.shard_map(
        local,
        mesh=mesh,
        in_specs=(
            P("lay", "blk", None),
            P("lay", "blk", None),
            P(None, "lay", "blk", None),
            P(None, "lay", "blk", None),
            P("lay", "blk"),
            P(None, "lay", "blk"),
            P(("blk", "lay")),
            P(("blk", "lay")),
            P(("blk", "lay")),
            P(None, ("blk", "lay")),
            P(("blk", "lay")),
            P(None, ("blk", "lay")),
            P(("blk", "lay")),
        ),
        out_specs=(P("lay", "blk", None), P(("blk", "lay"))),
        check_vma=False,
    )
```
